32 devices in a mesh: depth: 4 (over z), col: 2 (over y), row: 4 (over x, core).
Axes of the slice: x: 2, y: 2, z: 4, core: 2. Of those that a mesh axis runs over, the one named last changes fastest.
Arguments:
- weight: bfloat16 [3072, 3072], P(('row', 'depth'), 'col')
- rhs_stack: bfloat16 [3, 3072, 8192], P(None, ('row', 'depth'), 'col')
Outputs:
- output: bfloat16 [3, 3072, 8192], P(None, ('row', 'depth'), 'col')
All inputs are finite; a program needn't handle non-finite values.
Results may differ from the reference program's by a relative error of at most 0.001.
Values are sent between devices in bfloat16 or wider.
A program may use at most 1 GiB of HBM per device.

```python
import jax
import jax.numpy as jnp
from jax import lax

N = 3072
RHS_COLS = 8192


def setup_inputs(seed: int = 0) -> dict:
    base_key = jax.random.key(seed)
    key_w, key_x = jax.random.split(base_key)
    weight = jax.random.normal(key_w, (N, N), jnp.float32) * (N ** -0.5) + 2.0 / N
    rhs_stack = jax.random.normal(key_x, (3, N, RHS_COLS), jnp.float32) + 0.5
    return {"weight": weight.astype(jnp.bfloat16), "rhs_stack": rhs_stack.astype(jnp.bfloat16)}


def reference(weight, rhs_stack):
    def one_product(rhs_block):
        return jnp.dot(weight, rhs_block, preferred_element_type=jnp.float32).astype(jnp.bfloat16)
    return lax.map(one_product, rhs_stack)
```

```python
import functools

import jax
import jax.numpy as jnp
from jax import lax
from jax.experimental import pallas as pl
from jax.experimental.pallas import tpu as pltpu
from jax.sharding import PartitionSpec as P

MESH = pl.DeviceIdType.MESH
WIDTH = 256
AHEAD = 3
LAG = 4


def kernel(width, x_ref, a_ref, o_ref, xb, ab, yb, xa_send, xa_recv, xl_sem, xz_send, xz_recv, xt_recv, a_send, a_recv, al_sem, y_send, y_recv, yl_sem):
    z = lax.axis_index("depth")
    j = lax.axis_index("col")
    i = lax.axis_index("row")
    rhs, rows, cols = x_ref.shape
    quarter = cols // 4
    subs = quarter // width
    chunks = rhs * subs
    half = a_ref.shape[1]
    is_mid = (z + 1) // 2 == 1
    end = (z // 2) * 3
    near = 1 + z // 2
    peer = 3 - z
    core_i = i + 1 - 2 * (i % 2)
    x_i = (i + 2) % 4
    other_i = (core_i + 2) % 4

    def span(owner, sub):
        return pl.ds(pl.multiple_of(owner * quarter + sub * width, width), width)

    def a_unit(e, row, col):
        return ab.at[e, row, :, pl.ds(pl.multiple_of(col * half, half), half)]

    def remote(src, dst, send, recv, where):
        return pltpu.make_async_remote_copy(src_ref=src, dst_ref=dst, send_sem=send, recv_sem=recv, device_id=where, device_id_type=MESH)

    def wait_bytes(ref, sem):
        pltpu.make_async_copy(ref, ref, sem).wait()

    def swap_start(c):
        r, sub = c // subs, c % subs
        for to in (core_i, x_i, other_i):
            remote(x_ref.at[r, :, span(to, sub)], xb.at[c, i, z], xa_send, xa_recv.at[c, i], (z, j, to)).start()

    def own_start(c, to):
        r, sub = c // subs, c % subs
        remote(x_ref.at[r, :, span(i, sub)], xb.at[c, i, z], xz_send, xz_recv.at[c, z], (to, j, i)).start()

    def pass_on(c, to):
        for t in (core_i, x_i, other_i):
            wait_bytes(xb.at[c, t, z], xa_recv.at[c, t])
            remote(xb.at[c, t, z], xb.at[c, t, z], xz_send, xz_recv.at[c, z], (to, j, i)).start()

    def hop_start(c, layer, to):
        remote(xb.at[c, :, layer], xb.at[c, :, layer], xz_send, xz_recv.at[c, layer], (to, j, i)).start()

    def tails(h):
        return xb.at[chunks - 1, :, end, :, pl.ds(h * (width // 2), width // 2)]

    def hop_wait(c, layer):
        wait_bytes(xb.at[c, :, layer], xz_recv.at[c, layer])

    def a_start(src, e, row, col, where):
        remote(src, a_unit(e, row, col), a_send, a_recv.at[e, row, col], where).start()

    def a_wait(e, row, col):
        wait_bytes(a_unit(e, row, col), a_recv.at[e, row, col])

    barrier = pltpu.get_barrier_semaphore()
    for d in (1, 2, 3):
        pl.semaphore_signal(barrier, inc=1, device_id=(z, j, (i + d) % 4), device_id_type=MESH)

    @pl.when(is_mid)
    def _():
        pl.semaphore_signal(barrier, inc=1, device_id=(z, 1 - j, i), device_id_type=MESH)
        pl.semaphore_signal(barrier, inc=1, device_id=(peer, j, i), device_id_type=MESH)
        for t in range(4):
            pl.semaphore_signal(barrier, inc=1, device_id=(end, j, t), device_id_type=MESH)
        pl.semaphore_wait(barrier, 9)

    @pl.when(jnp.logical_not(is_mid))
    def _():
        for t in range(4):
            pl.semaphore_signal(barrier, inc=1, device_id=(near, j, t), device_id_type=MESH)
        pl.semaphore_wait(barrier, 7)

    @pl.when(jnp.logical_not(is_mid))
    def _():
        swap_start(0)
        a_start(a_ref, 0, i, j, (near, j, i))
        own_start(0, near)

        def issue(c, _):
            swap_start(c)
            own_start(c, near)
            return 0

        lax.fori_loop(1, AHEAD, issue, 0)

        def step(c, _):
            @pl.when(c + AHEAD < chunks)
            def _():
                issue(c + AHEAD, 0)

            pass_on(c, near)
            return 0

        lax.fori_loop(0, chunks, step, 0)
        wait_bytes(x_ref.at[:, :, pl.ds(0, 3 * quarter)], xa_send)
        wait_bytes(a_ref, a_send)
        wait_bytes(xb.at[:, :, 0], xz_send)
        wait_bytes(o_ref, y_recv)

    @pl.when(is_mid)
    def _():
        def a_fan(src, e, row):
            a_start(src, e, row, j, (z, 1 - j, i))
            a_start(src, e, row, j, (z, j, core_i))

        def issue(c, _):
            swap_start(c)
            own_start(c, peer)
            return 0

        issue(0, 0)
        a_fan(a_ref, 1, i)
        lax.fori_loop(1, AHEAD, issue, 0)
        a_start(a_ref, 1, i, j, (z, j, x_i))
        pltpu.make_async_copy(a_ref, a_unit(1, i, j), al_sem).start()

        def keep(c, _):
            pltpu.make_async_copy(x_ref.at[c // subs, :, span(i, c % subs)], xb.at[c, i, z], xl_sem).start()
            return 0

        lax.fori_loop(0, chunks, keep, 0)

        def forward(c, _):
            @pl.when(c + AHEAD < chunks)
            def _():
                issue(c + AHEAD, 0)

            pass_on(c, peer)
            return 0

        lax.fori_loop(0, AHEAD, forward, 0)

        def compute(c, at, size):
            r, sub = c // subs, c % subs
            cut = pl.ds(at, size)
            out = pl.ds(pl.multiple_of(i * quarter + sub * width + at, size), size)

            def unit(u, _):
                e, t = u // 4, u % 4
                block = xb[c, :, :, :, cut].reshape(16 * rows, size)
                yb[c, e, t, :, cut] = jnp.dot(ab[e, t], block, preferred_element_type=jnp.float32).astype(yb.dtype)
                layer = end + e * (z - end)
                mine = (e == 1) & (t == i)

                @pl.when(mine)
                def _():
                    pltpu.make_async_copy(yb.at[c, e, t, :, cut], o_ref.at[r, :, out], yl_sem).start()

                @pl.when(jnp.logical_not(mine))
                def _():
                    remote(yb.at[c, e, t, :, cut], o_ref.at[r, :, out], y_send, y_recv, (layer, j, t)).start()

                return 0

            lax.fori_loop(0, 8, unit, 0)

        def step(s, _):
            @pl.when(s < chunks)
            def _():
                hop_wait(s, end)

            @pl.when(s < chunks - 1)
            def _():
                hop_start(s, end, peer)

            @pl.when(s == chunks - 1)
            def _():
                for h in range(2):
                    remote(tails(h), tails(h), xz_send, xt_recv.at[h], (peer, j, i)).start()

            @pl.when(s + AHEAD < chunks)
            def _():
                forward(s + AHEAD, 0)

            @pl.when(s == 0)
            def _():
                a_wait(0, i, j)
                a_fan(a_unit(0, i, j), 0, i)
                a_start(a_unit(0, i, j), 0, i, j, (z, j, x_i))
                a_wait(1, x_i, j)
                a_fan(a_unit(1, x_i, j), 1, x_i)

            @pl.when(s == 1)
            def _():
                a_wait(1, i, 1 - j)
                a_start(a_unit(1, i, 1 - j), 1, i, 1 - j, (z, j, core_i))

            @pl.when(s == 2)
            def _():
                a_wait(0, x_i, j)
                a_fan(a_unit(0, x_i, j), 0, x_i)
                a_wait(0, i, 1 - j)
                a_start(a_unit(0, i, 1 - j), 0, i, 1 - j, (z, j, core_i))

            @pl.when(s == LAG - 1)
            def _():
                for e in (1, 0):
                    a_wait(e, x_i, 1 - j)
                    a_start(a_unit(e, x_i, 1 - j), e, x_i, 1 - j, (z, j, core_i))
                wait_bytes(a_unit(1, i, j), al_sem)
                wait_bytes(xb.at[:, 0, 0], xl_sem)
                for e in (1, 0):
                    for row in (core_i, other_i):
                        for col in range(2):
                            a_wait(e, row, col)

            @pl.when(s >= LAG)
            def _():
                hop_wait(s - LAG, peer)
                hop_wait(s - LAG, 3 - end)
                compute(s - LAG, 0, width)

            return 0

        lax.fori_loop(0, chunks + LAG - 1, step, 0)
        hop_wait(chunks - 1, peer)
        for h in range(2):
            wait_bytes(tails(h), xt_recv.at[h])
            compute(chunks - 1, h * (width // 2), width // 2)
        wait_bytes(x_ref.at[:, :, pl.ds(0, 3 * quarter)], xa_send)
        wait_bytes(ab.at[:, pl.ds(0, 3)], a_send)
        wait_bytes(ab.at[0, 0], a_send)
        wait_bytes(xb.at[:, :, pl.ds(0, 2)], xz_send)
        wait_bytes(yb.at[:, 0], y_send)
        wait_bytes(yb.at[:, 1, pl.ds(0, 3)], y_send)
        wait_bytes(yb.at[:, 1, 0], yl_sem)
        wait_bytes(o_ref.at[:, :, pl.ds(0, 3 * quarter)], y_recv)


def solution(mesh):
    def local_product(a, x):
        rhs, rows, cols = x.shape
        width = WIDTH
        while (cols // 4) % width:
            width //= 2
        chunks = rhs * (cols // 4 // width)
        dma = pltpu.SemaphoreType.DMA
        return pl.pallas_call(
            functools.partial(kernel, width),
            out_shape=pltpu.VMEM(x.shape, x.dtype),
            in_specs=[pl.BlockSpec(memory_space=pltpu.HBM)] * 2,
            out_specs=pl.BlockSpec(memory_space=pltpu.VMEM),
            scratch_shapes=[
                pltpu.VMEM((chunks, 4, 4, rows, width), x.dtype),
                pltpu.VMEM((2, 4, rows, 2 * a.shape[1]), a.dtype),
                pltpu.VMEM((chunks, 2, 4, rows, width), x.dtype),
                dma, dma((chunks, 4)), dma,
                dma, dma((chunks, 4)), dma((2,)),
                dma, dma((2, 4, 2)), dma,
                dma, dma, dma,
            ],
            compiler_params=pltpu.CompilerParams(collective_id=0, has_side_effects=True, vmem_limit_bytes=int(56.5 * 2**20)),
        )(x, a)

    return jax.shard_map(local_product, mesh=mesh, in_specs=(P(("row", "depth"), "col"), P(None, ("row", "depth"), "col")), out_specs=P(None, ("row", "depth"), "col"), check_vma=False)
```

```python
import functools

import jax
import jax.numpy as jnp
from jax import lax
from jax.experimental import pallas as pl
from jax.experimental.pallas import tpu as pltpu
from jax.sharding import PartitionSpec as P

MESH = pl.DeviceIdType.MESH
WIDTH = 256
AHEAD = 3
LAG = 4


def kernel(width, x_ref, a_ref, o_ref, xb, ab, yb, xa_send, xa_recv, xl_sem, xz_send, xz_recv, xt_recv, a_send, a_recv, al_sem, y_send, y_recv, yl_sem, ready):
    z = lax.axis_index("depth")
    j = lax.axis_index("col")
    i = lax.axis_index("row")
    rhs, rows, cols = x_ref.shape
    quarter = cols // 4
    subs = quarter // width
    chunks = rhs * subs
    half = a_ref.shape[1]
    is_mid = (z + 1) // 2 == 1
    end = (z // 2) * 3
    near = 1 + z // 2
    peer = 3 - z
    core_i = i + 1 - 2 * (i % 2)
    x_i = (i + 2) % 4
    other_i = (core_i + 2) % 4

    def span(owner, sub):
        return pl.ds(pl.multiple_of(owner * quarter + sub * width, width), width)

    def a_unit(e, row, col):
        return ab.at[e, row, :, pl.ds(pl.multiple_of(col * half, half), half)]

    def remote(src, dst, send, recv, where):
        return pltpu.make_async_remote_copy(src_ref=src, dst_ref=dst, send_sem=send, recv_sem=recv, device_id=where, device_id_type=MESH)

    def wait_bytes(ref, sem):
        pltpu.make_async_copy(ref, ref, sem).wait()

    def swap_start(c):
        r, sub = c // subs, c % subs
        for to in (core_i, x_i, other_i):
            remote(x_ref.at[r, :, span(to, sub)], xb.at[c, i, z], xa_send, xa_recv.at[c, i], (z, j, to)).start()

    def own_start(c, to):
        r, sub = c // subs, c % subs
        remote(x_ref.at[r, :, span(i, sub)], xb.at[c, i, z], xz_send, xz_recv.at[c, z], (to, j, i)).start()

    def pass_on(c, to):
        for t in (core_i, x_i, other_i):
            wait_bytes(xb.at[c, t, z], xa_recv.at[c, t])
            remote(xb.at[c, t, z], xb.at[c, t, z], xz_send, xz_recv.at[c, z], (to, j, i)).start()

    def hop_start(c, layer, to):
        remote(xb.at[c, :, layer], xb.at[c, :, layer], xz_send, xz_recv.at[c, layer], (to, j, i)).start()

    def tails(h):
        return xb.at[chunks - 1, :, end, :, pl.ds(h * (width // 2), width // 2)]

    def hop_wait(c, layer):
        wait_bytes(xb.at[c, :, layer], xz_recv.at[c, layer])

    def a_start(src, e, row, col, where):
        remote(src, a_unit(e, row, col), a_send, a_recv.at[e, row, col], where).start()

    def a_wait(e, row, col):
        wait_bytes(a_unit(e, row, col), a_recv.at[e, row, col])

    barrier = pltpu.get_barrier_semaphore()
    for d in (1, 2, 3):
        pl.semaphore_signal(barrier, inc=1, device_id=(z, j, (i + d) % 4), device_id_type=MESH)

    @pl.when(is_mid)
    def _():
        pl.semaphore_signal(barrier, inc=1, device_id=(z, 1 - j, i), device_id_type=MESH)
        pl.semaphore_signal(barrier, inc=1, device_id=(peer, j, i), device_id_type=MESH)
        for t in range(4):
            pl.semaphore_signal(barrier, inc=1, device_id=(end, j, t), device_id_type=MESH)
        pl.semaphore_wait(barrier, 5)

    @pl.when(jnp.logical_not(is_mid))
    def _():
        pl.semaphore_wait(barrier, 7)

    @pl.when(jnp.logical_not(is_mid))
    def _():
        swap_start(0)
        a_start(a_ref, 0, i, j, (near, j, i))
        own_start(0, near)
        for t in range(4):
            pl.semaphore_signal(ready, inc=1, device_id=(near, j, t), device_id_type=MESH)

        def issue(c, _):
            swap_start(c)
            own_start(c, near)
            return 0

        lax.fori_loop(1, AHEAD, issue, 0)

        def step(c, _):
            @pl.when(c + AHEAD < chunks)
            def _():
                issue(c + AHEAD, 0)

            pass_on(c, near)
            return 0

        lax.fori_loop(0, chunks, step, 0)
        wait_bytes(x_ref.at[:, :, pl.ds(0, 3 * quarter)], xa_send)
        wait_bytes(a_ref, a_send)
        wait_bytes(xb.at[:, :, 0], xz_send)
        wait_bytes(o_ref, y_recv)

    @pl.when(is_mid)
    def _():
        def a_fan(src, e, row):
            a_start(src, e, row, j, (z, 1 - j, i))
            a_start(src, e, row, j, (z, j, core_i))

        def issue(c, _):
            swap_start(c)
            own_start(c, peer)
            return 0

        issue(0, 0)
        a_fan(a_ref, 1, i)
        lax.fori_loop(1, AHEAD, issue, 0)
        a_start(a_ref, 1, i, j, (z, j, x_i))
        pltpu.make_async_copy(a_ref, a_unit(1, i, j), al_sem).start()

        def keep(c, _):
            pltpu.make_async_copy(x_ref.at[c // subs, :, span(i, c % subs)], xb.at[c, i, z], xl_sem).start()
            return 0

        lax.fori_loop(0, chunks, keep, 0)

        def forward(c, _):
            @pl.when(c + AHEAD < chunks)
            def _():
                issue(c + AHEAD, 0)

            pass_on(c, peer)
            return 0

        lax.fori_loop(0, AHEAD, forward, 0)

        def compute(c, at, size):
            r, sub = c // subs, c % subs
            cut = pl.ds(at, size)
            out = pl.ds(pl.multiple_of(i * quarter + sub * width + at, size), size)

            def unit(u, _):
                e, t = u // 4, u % 4
                block = xb[c, :, :, :, cut].reshape(16 * rows, size)
                yb[c, e, t, :, cut] = jnp.dot(ab[e, t], block, preferred_element_type=jnp.float32).astype(yb.dtype)
                layer = end + e * (z - end)
                mine = (e == 1) & (t == i)

                @pl.when(mine)
                def _():
                    pltpu.make_async_copy(yb.at[c, e, t, :, cut], o_ref.at[r, :, out], yl_sem).start()

                @pl.when(jnp.logical_not(mine))
                def _():
                    remote(yb.at[c, e, t, :, cut], o_ref.at[r, :, out], y_send, y_recv, (layer, j, t)).start()

                return 0

            lax.fori_loop(0, 8, unit, 0)

        def step(s, _):
            @pl.when(s < chunks)
            def _():
                hop_wait(s, end)

            @pl.when(s < chunks - 1)
            def _():
                hop_start(s, end, peer)

            @pl.when(s == chunks - 1)
            def _():
                for h in range(2):
                    remote(tails(h), tails(h), xz_send, xt_recv.at[h], (peer, j, i)).start()

            @pl.when(s == 0)
            def _():
                forward(AHEAD, 0)

            @pl.when((s >= AHEAD) & (s + 1 < chunks))
            def _():
                forward(s + 1, 0)

            @pl.when(s == 0)
            def _():
                a_wait(0, i, j)
                a_fan(a_unit(0, i, j), 0, i)
                a_start(a_unit(0, i, j), 0, i, j, (z, j, x_i))
                a_wait(1, x_i, j)
                a_fan(a_unit(1, x_i, j), 1, x_i)

            @pl.when(s == 1)
            def _():
                a_wait(1, i, 1 - j)
                a_start(a_unit(1, i, 1 - j), 1, i, 1 - j, (z, j, core_i))

            @pl.when(s == 2)
            def _():
                a_wait(0, x_i, j)
                a_fan(a_unit(0, x_i, j), 0, x_i)
                a_wait(0, i, 1 - j)
                a_start(a_unit(0, i, 1 - j), 0, i, 1 - j, (z, j, core_i))

            @pl.when(s == LAG - 1)
            def _():
                for e in (1, 0):
                    a_wait(e, x_i, 1 - j)
                    a_start(a_unit(e, x_i, 1 - j), e, x_i, 1 - j, (z, j, core_i))
                wait_bytes(a_unit(1, i, j), al_sem)
                pl.semaphore_wait(ready, 4)
                wait_bytes(xb.at[:, 0, 0], xl_sem)
                for e in (1, 0):
                    for row in (core_i, other_i):
                        for col in range(2):
                            a_wait(e, row, col)

            @pl.when(s >= LAG)
            def _():
                hop_wait(s - LAG, peer)
                hop_wait(s - LAG, 3 - end)
                compute(s - LAG, 0, width)

            return 0

        lax.fori_loop(0, chunks + LAG - 1, step, 0)
        hop_wait(chunks - 1, peer)
        for h in range(2):
            wait_bytes(tails(h), xt_recv.at[h])
            compute(chunks - 1, h * (width // 2), width // 2)
        wait_bytes(x_ref.at[:, :, pl.ds(0, 3 * quarter)], xa_send)
        wait_bytes(ab.at[:, pl.ds(0, 3)], a_send)
        wait_bytes(ab.at[0, 0], a_send)
        wait_bytes(xb.at[:, :, pl.ds(0, 2)], xz_send)
        wait_bytes(yb.at[:, 0], y_send)
        wait_bytes(yb.at[:, 1, pl.ds(0, 3)], y_send)
        wait_bytes(yb.at[:, 1, 0], yl_sem)
        wait_bytes(o_ref.at[:, :, pl.ds(0, 3 * quarter)], y_recv)


def solution(mesh):
    def local_product(a, x):
        rhs, rows, cols = x.shape
        width = WIDTH
        while (cols // 4) % width:
            width //= 2
        chunks = rhs * (cols // 4 // width)
        dma = pltpu.SemaphoreType.DMA
        return pl.pallas_call(
            functools.partial(kernel, width),
            out_shape=pltpu.VMEM(x.shape, x.dtype),
            in_specs=[pl.BlockSpec(memory_space=pltpu.HBM)] * 2,
            out_specs=pl.BlockSpec(memory_space=pltpu.VMEM),
            scratch_shapes=[
                pltpu.VMEM((chunks, 4, 4, rows, width), x.dtype),
                pltpu.VMEM((2, 4, rows, 2 * a.shape[1]), a.dtype),
                pltpu.VMEM((chunks, 2, 4, rows, width), x.dtype),
                dma, dma((chunks, 4)), dma,
                dma, dma((chunks, 4)), dma((2,)),
                dma, dma((2, 4, 2)), dma,
                dma, dma, dma, pltpu.SemaphoreType.REGULAR,
            ],
            compiler_params=pltpu.CompilerParams(collective_id=0, has_side_effects=True, vmem_limit_bytes=int(56.5 * 2**20)),
        )(x, a)

    return jax.shard_map(local_product, mesh=mesh, in_specs=(P(("row", "depth"), "col"), P(None, ("row", "depth"), "col")), out_specs=P(None, ("row", "depth"), "col"), check_vma=False)
```

```python
import functools

import jax
import jax.numpy as jnp
from jax import lax
from jax.experimental import pallas as pl
from jax.experimental.pallas import tpu as pltpu
from jax.sharding import PartitionSpec as P

MESH = pl.DeviceIdType.MESH
WIDTH = 256
AHEAD = 3
LAG = 4


def kernel(width, x_ref, a_ref, o_ref, xb, ab, yb, acc, xa_send, xa_recv, xl_sem, xz_send, xz_recv, xt_recv, a_send, a_recv, al_sem, y_send, y_recv, yl_sem, ready_core, ready_x, ready_y, ready):
    z = lax.axis_index("depth")
    j = lax.axis_index("col")
    i = lax.axis_index("row")
    rhs, rows, cols = x_ref.shape
    quarter = cols // 4
    subs = quarter // width
    chunks = rhs * subs
    half = a_ref.shape[1]
    is_mid = (z + 1) // 2 == 1
    end = (z // 2) * 3
    near = 1 + z // 2
    peer = 3 - z
    core_i = i + 1 - 2 * (i % 2)
    x_i = (i + 2) % 4
    other_i = (core_i + 2) % 4

    def span(owner, sub):
        return pl.ds(pl.multiple_of(owner * quarter + sub * width, width), width)

    def a_unit(e, row, col):
        return ab.at[e, row, :, pl.ds(pl.multiple_of(col * half, half), half)]

    def remote(src, dst, send, recv, where):
        return pltpu.make_async_remote_copy(src_ref=src, dst_ref=dst, send_sem=send, recv_sem=recv, device_id=where, device_id_type=MESH)

    def wait_bytes(ref, sem):
        pltpu.make_async_copy(ref, ref, sem).wait()

    def swap_start(c):
        r, sub = c // subs, c % subs
        for to in (core_i, x_i, other_i):
            remote(x_ref.at[r, :, span(to, sub)], xb.at[c, i, z], xa_send, xa_recv.at[c, i], (z, j, to)).start()

    def own_start(c, to):
        r, sub = c // subs, c % subs
        remote(x_ref.at[r, :, span(i, sub)], xb.at[c, i, z], xz_send, xz_recv.at[c, z], (to, j, i)).start()

    def pass_on(c, to):
        for t in (core_i, x_i, other_i):
            wait_bytes(xb.at[c, t, z], xa_recv.at[c, t])
            remote(xb.at[c, t, z], xb.at[c, t, z], xz_send, xz_recv.at[c, z], (to, j, i)).start()

    def hop_start(c, layer, to):
        remote(xb.at[c, :, layer], xb.at[c, :, layer], xz_send, xz_recv.at[c, layer], (to, j, i)).start()

    last, narrow = chunks - 1, width // 2

    def tail_part(n):
        if n == 0:
            return xb.at[last, :, end, :, pl.ds(0, narrow)]
        return xb.at[last, n - 1, end, :, pl.ds(narrow, narrow)]

    def tail_start(h):
        for t in (core_i, x_i, other_i):
            if h == 0:
                wait_bytes(xb.at[last, t, z], xa_recv.at[last, t])
            part = xb.at[last, t, z, :, pl.ds(h * narrow, narrow)]
            remote(part, part, xz_send, xt_recv.at[5 + h], (peer, j, i)).start()
        for n in (range(1, 5) if h else range(1)):
            remote(tail_part(n), tail_part(n), xz_send, xt_recv.at[n], (peer, j, i)).start()

    def hop_wait(c, layer):
        wait_bytes(xb.at[c, :, layer], xz_recv.at[c, layer])

    def a_start(src, e, row, col, where):
        remote(src, a_unit(e, row, col), a_send, a_recv.at[e, row, col], where).start()

    def a_wait(e, row, col):
        wait_bytes(a_unit(e, row, col), a_recv.at[e, row, col])

    def notify(sem, where):
        pl.semaphore_signal(sem, inc=1, device_id=where, device_id_type=MESH)

    barrier = pltpu.get_barrier_semaphore()

    @pl.when(is_mid)
    def _():
        notify(barrier, (peer, j, i))

        @pl.when(i % 2 == 0)
        def _():
            notify(barrier, (z, j, core_i))

        @pl.when(i < 2)
        def _():
            for to in (x_i, other_i):
                notify(barrier, (z, j, to))

        @pl.when(j == 0)
        def _():
            notify(barrier, (z, 1, i))

        pl.semaphore_wait(barrier, 1 + i % 2 + i // 2 * 2 + j)

    @pl.when(jnp.logical_not(is_mid))
    def _():
        for d in (1, 2, 3):
            notify(barrier, (z, j, (i + d) % 4))
        pl.semaphore_wait(barrier, 7)

    @pl.when(jnp.logical_not(is_mid))
    def _():
        swap_start(0)
        a_start(a_ref, 0, i, j, (near, j, i))
        own_start(0, near)
        for t in range(4):
            notify(ready, (near, j, t))

        def issue(c, _):
            swap_start(c)
            own_start(c, near)
            return 0

        lax.fori_loop(1, AHEAD, issue, 0)

        def step(c, _):
            @pl.when(c + AHEAD < chunks)
            def _():
                issue(c + AHEAD, 0)

            pass_on(c, near)
            return 0

        lax.fori_loop(0, chunks, step, 0)
        wait_bytes(x_ref.at[:, :, pl.ds(0, 3 * quarter)], xa_send)
        wait_bytes(a_ref, a_send)
        wait_bytes(xb.at[:, :, 0], xz_send)
        wait_bytes(o_ref, y_recv)

    @pl.when(is_mid)
    def _():
        def a_fan(src, e, row):
            a_start(src, e, row, j, (z, 1 - j, i))
            a_start(src, e, row, j, (z, j, core_i))

        def issue(c, _):
            swap_start(c)
            own_start(c, peer)
            return 0

        def first(c, _):
            own_start(c, peer)
            return 0

        def swap_more(c, _):
            swap_start(c)
            return 0

        lax.fori_loop(0, AHEAD, first, 0)
        for t in range(4):
            notify(barrier, (end, j, t))

        @pl.when(i % 2 == 1)
        def _():
            notify(ready_core, (z, j, core_i))

        @pl.when(i >= 2)
        def _():
            for to in (x_i, other_i):
                notify(ready_x, (z, j, to))

        @pl.when(j == 1)
        def _():
            notify(ready_y, (z, 0, i))

        @pl.when(i % 2 == 0)
        def _():
            pl.semaphore_wait(ready_core, 1)

        @pl.when(i < 2)
        def _():
            pl.semaphore_wait(ready_x, 2)

        swap_start(0)

        @pl.when(j == 0)
        def _():
            pl.semaphore_wait(ready_y, 1)

        a_fan(a_ref, 1, i)
        lax.fori_loop(1, AHEAD, swap_more, 0)
        a_start(a_ref, 1, i, j, (z, j, x_i))
        pltpu.make_async_copy(a_ref, a_unit(1, i, j), al_sem).start()

        def keep(c, _):
            pltpu.make_async_copy(x_ref.at[c // subs, :, span(i, c % subs)], xb.at[c, i, z], xl_sem).start()
            return 0

        lax.fori_loop(0, chunks, keep, 0)

        def forward(c, _):
            @pl.when(c + AHEAD < chunks)
            def _():
                issue(c + AHEAD, 0)

            pass_on(c, peer)
            return 0

        lax.fori_loop(0, AHEAD, forward, 0)

        def compute(c, at, size, lo=0, hi=8, done=0):
            r, sub = c // subs, c % subs
            cut = pl.ds(at, size)
            out = pl.ds(pl.multiple_of(i * quarter + sub * width + at, size), size)

            def unit(u, _):
                e, t = u // 4, u % 4
                block = xb[c, done:, :, :, cut].reshape((4 - done) * 4 * rows, size)
                total = jnp.dot(ab[e, t, :, done * 4 * rows :], block, preferred_element_type=jnp.float32)
                if done:
                    total = total + acc[t]
                yb[c, e, t, :, cut] = total.astype(yb.dtype)
                layer = end + e * (z - end)
                mine = (e == 1) & (t == i)

                @pl.when(mine)
                def _():
                    pltpu.make_async_copy(yb.at[c, e, t, :, cut], o_ref.at[r, :, out], yl_sem).start()

                @pl.when(jnp.logical_not(mine))
                def _():
                    remote(yb.at[c, e, t, :, cut], o_ref.at[r, :, out], y_send, y_recv, (layer, j, t)).start()

                return 0

            lax.fori_loop(lo, hi, unit, 0)

        def step(s, _):
            @pl.when(s < chunks)
            def _():
                hop_wait(s, end)

            @pl.when(s < chunks - 1)
            def _():
                hop_start(s, end, peer)

            @pl.when(s == last)
            def _():
                tail_start(0)

            @pl.when((s == last) & (i % 2 == 0))
            def _():
                tail_start(1)

            @pl.when(s == 0)
            def _():
                forward(AHEAD, 0)

            @pl.when((s >= AHEAD) & (s + 1 < last))
            def _():
                forward(s + 1, 0)

            @pl.when(s == 0)
            def _():
                a_wait(0, i, j)
                a_fan(a_unit(0, i, j), 0, i)
                a_start(a_unit(0, i, j), 0, i, j, (z, j, x_i))
                a_wait(1, x_i, j)
                a_fan(a_unit(1, x_i, j), 1, x_i)

            @pl.when(s == 1)
            def _():
                a_wait(1, i, 1 - j)
                a_start(a_unit(1, i, 1 - j), 1, i, 1 - j, (z, j, core_i))

            @pl.when(s == 2)
            def _():
                a_wait(0, x_i, j)
                a_fan(a_unit(0, x_i, j), 0, x_i)
                a_wait(0, i, 1 - j)
                a_start(a_unit(0, i, 1 - j), 0, i, 1 - j, (z, j, core_i))

            @pl.when(s == LAG - 1)
            def _():
                for e in (1, 0):
                    a_wait(e, x_i, 1 - j)
                    a_start(a_unit(e, x_i, 1 - j), e, x_i, 1 - j, (z, j, core_i))
                wait_bytes(a_unit(1, i, j), al_sem)
                pl.semaphore_wait(ready, 4)
                wait_bytes(xb.at[:, 0, 0], xl_sem)
                for e in (1, 0):
                    for row in (core_i, other_i):
                        for col in range(2):
                            a_wait(e, row, col)

            @pl.when(s >= LAG)
            def _():
                hop_wait(s - LAG, peer)
                hop_wait(s - LAG, 3 - end)
                compute(s - LAG, 0, width)

            return 0

        lax.fori_loop(0, chunks + LAG - 1, step, 0)
        wait_bytes(xb.at[last, 0, peer], xz_recv.at[last, peer])
        wait_bytes(xb.at[last, pl.ds(0, 3), peer, :, pl.ds(0, narrow)], xt_recv.at[5])
        wait_bytes(tail_part(0), xt_recv.at[0])
        compute(last, 0, narrow, 0, 4)

        @pl.when(i % 2 == 1)
        def _():
            tail_start(1)

        compute(last, 0, narrow, 4, 8)
        wait_bytes(xb.at[last, pl.ds(0, 3), peer, :, pl.ds(0, narrow)], xt_recv.at[6])
        for n in range(3):
            wait_bytes(tail_part(n + 1), xt_recv.at[n + 1])
            rhs_part = xb[last, n, :, :, pl.ds(narrow, narrow)].reshape(4 * rows, narrow)
            lhs_part = ab[0, :, :, 4 * rows * n : 4 * rows * (n + 1)].reshape(4 * rows, 4 * rows)
            sums = jnp.dot(lhs_part, rhs_part, preferred_element_type=jnp.float32).reshape(4, rows, narrow)
            acc[...] = sums if n == 0 else acc[...] + sums
        wait_bytes(tail_part(4), xt_recv.at[4])
        compute(last, narrow, narrow, 0, 4, 3)
        compute(last, narrow, narrow, 4, 8)
        wait_bytes(x_ref.at[:, :, pl.ds(0, 3 * quarter)], xa_send)
        wait_bytes(ab.at[:, pl.ds(0, 3)], a_send)
        wait_bytes(ab.at[0, 0], a_send)
        wait_bytes(xb.at[:, :, pl.ds(0, 2)], xz_send)
        wait_bytes(yb.at[:, 0], y_send)
        wait_bytes(yb.at[:, 1, pl.ds(0, 3)], y_send)
        wait_bytes(yb.at[:, 1, 0], yl_sem)
        wait_bytes(o_ref.at[:, :, pl.ds(0, 3 * quarter)], y_recv)


def solution(mesh):
    def local_product(a, x):
        rhs, rows, cols = x.shape
        width = WIDTH
        while (cols // 4) % width:
            width //= 2
        chunks = rhs * (cols // 4 // width)
        dma = pltpu.SemaphoreType.DMA
        return pl.pallas_call(
            functools.partial(kernel, width),
            out_shape=pltpu.VMEM(x.shape, x.dtype),
            in_specs=[pl.BlockSpec(memory_space=pltpu.HBM)] * 2,
            out_specs=pl.BlockSpec(memory_space=pltpu.VMEM),
            scratch_shapes=[
                pltpu.VMEM((chunks, 4, 4, rows, width), x.dtype),
                pltpu.VMEM((2, 4, rows, 2 * a.shape[1]), a.dtype),
                pltpu.VMEM((chunks, 2, 4, rows, width), x.dtype),
                pltpu.VMEM((4, rows, width // 2), jnp.float32),
                dma, dma((chunks, 4)), dma,
                dma, dma((chunks, 4)), dma((7,)),
                dma, dma((2, 4, 2)), dma,
                dma, dma, dma, pltpu.SemaphoreType.REGULAR, pltpu.SemaphoreType.REGULAR, pltpu.SemaphoreType.REGULAR, pltpu.SemaphoreType.REGULAR,
            ],
            compiler_params=pltpu.CompilerParams(collective_id=0, has_side_effects=True, vmem_limit_bytes=int(56.5 * 2**20)),
        )(x, a)

    return jax.shard_map(local_product, mesh=mesh, in_specs=(P(("row", "depth"), "col"), P(None, ("row", "depth"), "col")), out_specs=P(None, ("row", "depth"), "col"), check_vma=False)
```

```python
import functools

import jax
import jax.numpy as jnp
from jax import lax
from jax.experimental import pallas as pl
from jax.experimental.pallas import tpu as pltpu
from jax.sharding import PartitionSpec as P

MESH = pl.DeviceIdType.MESH
WIDTH = 256
AHEAD = 3
LAG = 4


def kernel(width, x_ref, a_ref, o_ref, xb, ab, yb, acc, xa_send, xa_first, xa_recv, xl_sem, xz_send, xe_recv, xp_recv, xt_recv, a_send, a_end, a_x, a_y, a_core, al_sem, y_send, y_recv, yl_sem, ready_core, ready_x, ready_y, ready):
    z = lax.axis_index("depth")
    j = lax.axis_index("col")
    i = lax.axis_index("row")
    rhs, rows, cols = x_ref.shape
    quarter = cols // 4
    subs = quarter // width
    chunks = rhs * subs
    half = a_ref.shape[1]
    is_mid = (z + 1) // 2 == 1
    end = (z // 2) * 3
    near = 1 + z // 2
    peer = 3 - z
    core_i = i + 1 - 2 * (i % 2)
    x_i = (i + 2) % 4
    other_i = (core_i + 2) % 4

    def span(owner, sub):
        return pl.ds(pl.multiple_of(owner * quarter + sub * width, width), width)

    def a_unit(e, row, col):
        return ab.at[e, row, :, pl.ds(pl.multiple_of(col * half, half), half)]

    def remote(src, dst, send, recv, where):
        return pltpu.make_async_remote_copy(src_ref=src, dst_ref=dst, send_sem=send, recv_sem=recv, device_id=where, device_id_type=MESH)

    def wait_bytes(ref, sem):
        pltpu.make_async_copy(ref, ref, sem).wait()

    def first_chunk(c):
        return isinstance(c, int) and c == 0

    def swap_start(c):
        r, sub = c // subs, c % subs
        arrived = xa_first.at[i] if first_chunk(c) else xa_recv.at[c]
        for to in (core_i, x_i, other_i):
            remote(x_ref.at[r, :, span(to, sub)], xb.at[c, i, z], xa_send, arrived, (z, j, to)).start()

    def own_start(c, to, arrived):
        r, sub = c // subs, c % subs
        remote(x_ref.at[r, :, span(i, sub)], xb.at[c, i, z], xz_send, arrived.at[c], (to, j, i)).start()

    def pass_on(c, to, arrived):
        if not first_chunk(c):
            wait_bytes(xb.at[c, pl.ds(0, 3), z], xa_recv.at[c])
        for t in (core_i, x_i, other_i):
            if first_chunk(c):
                wait_bytes(xb.at[c, t, z], xa_first.at[t])
            remote(xb.at[c, t, z], xb.at[c, t, z], xz_send, arrived.at[c], (to, j, i)).start()

    last, narrow = chunks - 1, width // 2

    def tail_part(n):
        if n == 0:
            return xb.at[last, :, end, :, pl.ds(0, narrow)]
        return xb.at[last, pl.ds(2 * n - 2, 2), end, :, pl.ds(narrow, narrow)]

    def tail_start(h):
        if h == 0:
            wait_bytes(xb.at[last, pl.ds(0, 3), z], xa_recv.at[last])
        part = xb.at[last, :, z, :, pl.ds(h * narrow, narrow)]
        remote(part, part, xz_send, xt_recv.at[h], (peer, j, i)).start()
        for n in ((1, 2) if h else (0,)):
            remote(tail_part(n), tail_part(n), xz_send, xt_recv.at[n], (peer, j, i)).start()

    def a_start(src, e, row, col, arrived, where):
        remote(src, a_unit(e, row, col), a_send, arrived, where).start()

    def notify(sem, where):
        pl.semaphore_signal(sem, inc=1, device_id=where, device_id_type=MESH)

    barrier = pltpu.get_barrier_semaphore()

    @pl.when(is_mid)
    def _():
        notify(barrier, (peer, j, i))

        @pl.when(i % 2 == 0)
        def _():
            notify(barrier, (z, j, core_i))

        @pl.when(i < 2)
        def _():
            for to in (x_i, other_i):
                notify(barrier, (z, j, to))

        @pl.when(j == 0)
        def _():
            notify(barrier, (z, 1, i))

        pl.semaphore_wait(barrier, 1 + i % 2 + i // 2 * 2 + j)

    @pl.when(jnp.logical_not(is_mid))
    def _():
        for d in (1, 2, 3):
            notify(barrier, (z, j, (i + d) % 4))
        pl.semaphore_wait(barrier, 7)

    @pl.when(jnp.logical_not(is_mid))
    def _():
        swap_start(0)
        a_start(a_ref, 0, i, j, a_end, (near, j, i))
        own_start(0, near, xe_recv)
        for t in range(4):
            notify(ready, (near, j, t))

        def issue(c, _):
            swap_start(c)
            own_start(c, near, xe_recv)
            return 0

        lax.fori_loop(1, AHEAD, issue, 0)

        def step(c, _):
            @pl.when(c + AHEAD < chunks)
            def _():
                issue(c + AHEAD, 0)

            pass_on(c, near, xe_recv)
            return 0

        step(0, 0)
        lax.fori_loop(1, chunks, step, 0)
        wait_bytes(x_ref.at[:, :, pl.ds(0, 3 * quarter)], xa_send)
        wait_bytes(a_ref, a_send)
        wait_bytes(xb.at[:, :, 0], xz_send)
        wait_bytes(o_ref, y_recv)

    @pl.when(is_mid)
    def _():
        def a_fan(src, e, row):
            a_start(src, e, row, j, a_y.at[e, 0 if row is i else 1], (z, 1 - j, i))
            a_start(src, e, row, j, a_core, (z, j, core_i))

        def issue(c, _):
            swap_start(c)

            @pl.when(c < last)
            def _():
                own_start(c, peer, xp_recv)

            return 0

        def first(c, _):
            own_start(c, peer, xp_recv)
            return 0

        def swap_more(c, _):
            swap_start(c)
            return 0

        lax.fori_loop(0, AHEAD, first, 0)
        for t in range(4):
            notify(barrier, (end, j, t))

        @pl.when(i % 2 == 1)
        def _():
            notify(ready_core, (z, j, core_i))

        @pl.when(i >= 2)
        def _():
            for to in (x_i, other_i):
                notify(ready_x, (z, j, to))

        @pl.when(j == 1)
        def _():
            notify(ready_y, (z, 0, i))

        @pl.when(i % 2 == 0)
        def _():
            pl.semaphore_wait(ready_core, 1)

        @pl.when(i < 2)
        def _():
            pl.semaphore_wait(ready_x, 2)

        swap_start(0)

        @pl.when(j == 0)
        def _():
            pl.semaphore_wait(ready_y, 1)

        a_fan(a_ref, 1, i)
        lax.fori_loop(1, AHEAD, swap_more, 0)
        a_start(a_ref, 1, i, j, a_x.at[1], (z, j, x_i))
        pltpu.make_async_copy(a_ref, a_unit(1, i, j), al_sem).start()

        def keep(c, _):
            pltpu.make_async_copy(x_ref.at[c // subs, :, span(i, c % subs)], xb.at[c, i, z], xl_sem).start()
            return 0

        lax.fori_loop(0, chunks, keep, 0)

        def forward(c, _):
            @pl.when(c + AHEAD < chunks)
            def _():
                issue(c + AHEAD, 0)

            pass_on(c, peer, xp_recv)
            return 0

        forward(0, 0)
        lax.fori_loop(1, AHEAD, forward, 0)

        def compute(c, at, size, lo=0, hi=8, done=0):
            r, sub = c // subs, c % subs
            cut = pl.ds(at, size)
            out = pl.ds(pl.multiple_of(i * quarter + sub * width + at, size), size)

            def unit(u, _):
                e, t = u // 4, u % 4
                block = xb[c, done:, :, :, cut].reshape((4 - done) * 4 * rows, size)
                total = jnp.dot(ab[e, t, :, done * 4 * rows :], block, preferred_element_type=jnp.float32)
                if done:
                    total = total + acc[t]
                yb[c, e, t, :, cut] = total.astype(yb.dtype)
                layer = end + e * (z - end)
                mine = (e == 1) & (t == i)

                @pl.when(mine)
                def _():
                    pltpu.make_async_copy(yb.at[c, e, t, :, cut], o_ref.at[r, :, out], yl_sem).start()

                @pl.when(jnp.logical_not(mine))
                def _():
                    remote(yb.at[c, e, t, :, cut], o_ref.at[r, :, out], y_send, y_recv, (layer, j, t)).start()

                return 0

            lax.fori_loop(lo, hi, unit, 0)

        def step(s, _):
            @pl.when(s < chunks)
            def _():
                wait_bytes(xb.at[s, :, end], xe_recv.at[s])

            @pl.when(s < chunks - 1)
            def _():
                remote(xb.at[s, :, end], xb.at[s, :, end], xz_send, xp_recv.at[s], (peer, j, i)).start()

            @pl.when(s == last)
            def _():
                tail_start(0)

            @pl.when((s == last) & (i % 2 == 0))
            def _():
                tail_start(1)

            @pl.when(s == 0)
            def _():
                forward(AHEAD, 0)

            @pl.when((s >= AHEAD) & (s + 1 < last))
            def _():
                forward(s + 1, 0)

            @pl.when(s == 0)
            def _():
                wait_bytes(a_ref, a_end)
                a_fan(a_unit(0, i, j), 0, i)
                a_start(a_unit(0, i, j), 0, i, j, a_x.at[0], (z, j, x_i))
                wait_bytes(a_ref, a_x.at[1])
                a_fan(a_unit(1, x_i, j), 1, x_i)

            def a_turn(e, k):
                wait_bytes(a_ref, a_y.at[e, k])
                row = x_i if k else i
                a_start(a_unit(e, row, 1 - j), e, row, 1 - j, a_core, (z, j, core_i))

            @pl.when(s == 1)
            def _():
                a_turn(1, 0)

            @pl.when(s == 2)
            def _():
                wait_bytes(a_ref, a_x.at[0])
                a_fan(a_unit(0, x_i, j), 0, x_i)
                a_turn(0, 0)

            @pl.when(s == LAG - 1)
            def _():
                a_turn(1, 1)
                a_turn(0, 1)
                wait_bytes(a_unit(1, i, j), al_sem)
                pl.semaphore_wait(ready, 4)
                wait_bytes(xb.at[:, 0, 0], xl_sem)
                wait_bytes(ab.at[0], a_core)

            @pl.when(s >= LAG)
            def _():
                wait_bytes(xb.at[s - LAG, :, pl.ds(0, 2)], xp_recv.at[s - LAG])
                compute(s - LAG, 0, width)

            return 0

        lax.fori_loop(0, chunks + LAG - 1, step, 0)
        wait_bytes(xb.at[pl.ds(0, 8), 0, 0, :, pl.ds(0, narrow)], xt_recv.at[0])
        compute(last, 0, narrow, 0, 5)

        @pl.when(i % 2 == 1)
        def _():
            tail_start(1)

        compute(last, 0, narrow, 5, 8)
        wait_bytes(xb.at[pl.ds(0, 6), 0, 0, :, pl.ds(0, narrow)], xt_recv.at[1])
        rhs_part = xb[last, :2, :, :, pl.ds(narrow, narrow)].reshape(8 * rows, narrow)
        lhs_part = ab[0, :, :, : 8 * rows].reshape(4 * rows, 8 * rows)
        acc[...] = jnp.dot(lhs_part, rhs_part, preferred_element_type=jnp.float32).reshape(4, rows, narrow)
        wait_bytes(tail_part(2), xt_recv.at[2])
        compute(last, narrow, narrow, 0, 4, 2)
        compute(last, narrow, narrow, 4, 8)
        wait_bytes(x_ref.at[:, :, pl.ds(0, 3 * quarter)], xa_send)
        wait_bytes(ab.at[:, pl.ds(0, 3)], a_send)
        wait_bytes(ab.at[0, 0], a_send)
        wait_bytes(xb.at[:, :, pl.ds(0, 2)], xz_send)
        wait_bytes(yb.at[:, 0], y_send)
        wait_bytes(yb.at[:, 1, pl.ds(0, 3)], y_send)
        wait_bytes(yb.at[:, 1, 0], yl_sem)
        wait_bytes(o_ref.at[:, :, pl.ds(0, 3 * quarter)], y_recv)


def solution(mesh):
    def local_product(a, x):
        rhs, rows, cols = x.shape
        width = WIDTH
        while (cols // 4) % width:
            width //= 2
        chunks = rhs * (cols // 4 // width)
        dma = pltpu.SemaphoreType.DMA
        return pl.pallas_call(
            functools.partial(kernel, width),
            out_shape=pltpu.VMEM(x.shape, x.dtype),
            in_specs=[pl.BlockSpec(memory_space=pltpu.HBM)] * 2,
            out_specs=pl.BlockSpec(memory_space=pltpu.VMEM),
            scratch_shapes=[
                pltpu.VMEM((chunks, 4, 4, rows, width), x.dtype),
                pltpu.VMEM((2, 4, rows, 2 * a.shape[1]), a.dtype),
                pltpu.VMEM((chunks, 2, 4, rows, width), x.dtype),
                pltpu.VMEM((4, rows, width // 2), jnp.float32),
                dma, dma((4,)), dma((chunks,)), dma,
                dma, dma((chunks,)), dma((chunks,)), dma((3,)),
                dma, dma, dma((2,)), dma((2, 2)), dma, dma,
                dma, dma, dma, pltpu.SemaphoreType.REGULAR, pltpu.SemaphoreType.REGULAR, pltpu.SemaphoreType.REGULAR, pltpu.SemaphoreType.REGULAR,
            ],
            compiler_params=pltpu.CompilerParams(collective_id=0, has_side_effects=True, vmem_limit_bytes=int(56.5 * 2**20)),
        )(x, a)

    return jax.shard_map(local_product, mesh=mesh, in_specs=(P(("row", "depth"), "col"), P(None, ("row", "depth"), "col")), out_specs=P(None, ("row", "depth"), "col"), check_vma=False)
```

```python
import functools

import jax
import jax.numpy as jnp
from jax import lax
from jax.experimental import pallas as pl
from jax.experimental.pallas import tpu as pltpu
from jax.sharding import PartitionSpec as P

MESH = pl.DeviceIdType.MESH
WIDTH = 256
AHEAD = 3
LAG = 4


def kernel(width, x_ref, a_ref, o_ref, xb, ab, yb, acc, sent, xa_first, xa_recv, kept, xe_recv, xp_recv, xt_recv, a_end, a_x, a_y, a_core, y_recv, yl_sem, ready_core, ready_x, ready_y, ready):
    z = lax.axis_index("depth")
    j = lax.axis_index("col")
    i = lax.axis_index("row")
    rhs, rows, cols = x_ref.shape
    quarter = cols // 4
    subs = quarter // width
    chunks = rhs * subs
    last, narrow = chunks - 1, width // 2
    half = a_ref.shape[1]
    is_mid = (z + 1) // 2 == 1
    end = (z // 2) * 3
    near = 1 + z // 2
    peer = 3 - z
    core_i = i + 1 - 2 * (i % 2)
    x_i = (i + 2) % 4
    other_i = (core_i + 2) % 4

    def span(owner, sub):
        return pl.ds(pl.multiple_of(owner * quarter + sub * width, width), width)

    def a_unit(e, row, col):
        return ab.at[e, row, :, pl.ds(pl.multiple_of(col * half, half), half)]

    def remote(src, dst, send, recv, where):
        return pltpu.make_async_remote_copy(src_ref=src, dst_ref=dst, send_sem=send, recv_sem=recv, device_id=where, device_id_type=MESH)

    def wait_bytes(ref, sem):
        pltpu.make_async_copy(ref, ref, sem).wait()

    def early(c):
        return isinstance(c, int) and c < AHEAD

    def swap_slot(c):
        return xa_recv.at[c - 1 if early(c) else AHEAD - 1 + (c - AHEAD) // 2]

    def swap_start(c):
        r, sub = c // subs, c % subs
        arrived = xa_first.at[i] if early(c) and c == 0 else swap_slot(c)
        for to in (core_i, x_i, other_i):
            remote(x_ref.at[r, :, span(to, sub)], xb.at[c, i, z], sent, arrived, (z, j, to)).start()

    def own_start(c, to, arrived):
        r, sub = c // subs, c % subs
        remote(x_ref.at[r, :, span(i, sub)], xb.at[c, i, z], sent, arrived.at[c], (to, j, i)).start()

    def pass_on(c, to, arrived):
        if early(c):
            if c:
                wait_bytes(xb.at[c, pl.ds(0, 3), z], swap_slot(c))
        else:
            opens = (c - AHEAD) % 2 == 0

            @pl.when(jnp.logical_and(opens, c < last))
            def _():
                wait_bytes(xb.at[pl.ds(0, 2), pl.ds(0, 3), z], swap_slot(c))

            @pl.when(jnp.logical_and(opens, c == last))
            def _():
                wait_bytes(xb.at[c, pl.ds(0, 3), z], swap_slot(c))

        for t in (core_i, x_i, other_i):
            if early(c) and c == 0:
                wait_bytes(xb.at[c, t, z], xa_first.at[t])
            remote(xb.at[c, t, z], xb.at[c, t, z], sent, arrived.at[c], (to, j, i)).start()

    def tail_part(n):
        if n == 0:
            return xb.at[last, :, end, :, pl.ds(0, narrow)]
        return xb.at[last, pl.ds(2 * n - 2, 2), end, :, pl.ds(narrow, narrow)]

    def tail_start(h):
        if h == 0:
            wait_bytes(xb.at[last, pl.ds(0, 3), z], swap_slot(last))
        part = xb.at[last, :, z, :, pl.ds(h * narrow, narrow)]
        remote(part, part, sent, xt_recv.at[h], (peer, j, i)).start()
        for n in ((1, 2) if h else (0,)):
            remote(tail_part(n), tail_part(n), sent, xt_recv.at[n], (peer, j, i)).start()

    def a_start(src, e, row, col, arrived, where):
        remote(src, a_unit(e, row, col), sent, arrived, where).start()

    def notify(sem, where):
        pl.semaphore_signal(sem, inc=1, device_id=where, device_id_type=MESH)

    barrier = pltpu.get_barrier_semaphore()

    @pl.when(is_mid)
    def _():
        notify(barrier, (peer, j, i))

        @pl.when(i % 2 == 0)
        def _():
            notify(barrier, (z, j, core_i))

        @pl.when(i < 2)
        def _():
            for to in (x_i, other_i):
                notify(barrier, (z, j, to))

        @pl.when(j == 0)
        def _():
            notify(barrier, (z, 1, i))

        pl.semaphore_wait(barrier, 1 + i % 2 + i // 2 * 2 + j)

    @pl.when(jnp.logical_not(is_mid))
    def _():
        for d in (1, 2, 3):
            notify(barrier, (z, j, (i + d) % 4))
        pl.semaphore_wait(barrier, 7)

    @pl.when(jnp.logical_not(is_mid))
    def _():
        swap_start(0)
        a_start(a_ref, 0, i, j, a_end, (near, j, i))
        own_start(0, near, xe_recv)
        for t in range(4):
            notify(ready, (near, j, t))

        def issue(c, _):
            swap_start(c)
            own_start(c, near, xe_recv)
            return 0

        for c in range(1, AHEAD):
            issue(c, 0)

        def step(c, _):
            @pl.when(c + AHEAD < chunks)
            def _():
                issue(c + AHEAD, 0)

            pass_on(c, near, xe_recv)
            return 0

        for c in range(AHEAD):
            step(c, 0)
        lax.fori_loop(AHEAD, chunks, step, 0)
        wait_bytes(x_ref.at[:, :, pl.ds(0, 3 * quarter)], sent)
        wait_bytes(a_ref, sent)
        wait_bytes(xb.at[:, :, 0], sent)
        wait_bytes(o_ref, y_recv)

    @pl.when(is_mid)
    def _():
        def a_fan(src, e, row):
            a_start(src, e, row, j, a_y.at[e, 0 if row is i else 1], (z, 1 - j, i))
            a_start(src, e, row, j, a_core, (z, j, core_i))

        def issue(c, _):
            swap_start(c)

            @pl.when(c < last)
            def _():
                own_start(c, peer, xp_recv)

            return 0

        def first(c, _):
            own_start(c, peer, xp_recv)
            return 0

        lax.fori_loop(0, AHEAD, first, 0)
        for t in range(4):
            notify(barrier, (end, j, t))

        @pl.when(i % 2 == 1)
        def _():
            notify(ready_core, (z, j, core_i))

        @pl.when(i >= 2)
        def _():
            for to in (x_i, other_i):
                notify(ready_x, (z, j, to))

        @pl.when(j == 1)
        def _():
            notify(ready_y, (z, 0, i))

        @pl.when(i % 2 == 0)
        def _():
            pl.semaphore_wait(ready_core, 1)

        @pl.when(i < 2)
        def _():
            pl.semaphore_wait(ready_x, 2)

        swap_start(0)

        @pl.when(j == 0)
        def _():
            pl.semaphore_wait(ready_y, 1)

        a_fan(a_ref, 1, i)
        for c in range(1, AHEAD):
            swap_start(c)
        a_start(a_ref, 1, i, j, a_x.at[1], (z, j, x_i))
        pltpu.make_async_copy(a_ref, a_unit(1, i, j), kept).start()

        def keep(c, _):
            pltpu.make_async_copy(x_ref.at[c // subs, :, span(i, c % subs)], xb.at[c, i, z], kept).start()
            return 0

        lax.fori_loop(0, chunks, keep, 0)

        def forward(c, _):
            @pl.when(c + AHEAD < chunks)
            def _():
                issue(c + AHEAD, 0)

            pass_on(c, peer, xp_recv)
            return 0

        for c in range(AHEAD):
            forward(c, 0)

        def compute(c, at, size, lo=0, hi=8, done=0):
            r, sub = c // subs, c % subs
            cut = pl.ds(at, size)
            out = pl.ds(pl.multiple_of(i * quarter + sub * width + at, size), size)

            def unit(u, _):
                e, t = u // 4, u % 4
                block = xb[c, done:, :, :, cut].reshape((4 - done) * 4 * rows, size)
                total = jnp.dot(ab[e, t, :, done * 4 * rows :], block, preferred_element_type=jnp.float32)
                if done:
                    total = total + acc[t]
                yb[c, e, t, :, cut] = total.astype(yb.dtype)
                layer = end + e * (z - end)
                mine = (e == 1) & (t == i)

                @pl.when(mine)
                def _():
                    pltpu.make_async_copy(yb.at[c, e, t, :, cut], o_ref.at[r, :, out], yl_sem).start()

                @pl.when(jnp.logical_not(mine))
                def _():
                    remote(yb.at[c, e, t, :, cut], o_ref.at[r, :, out], sent, y_recv, (layer, j, t)).start()

                return 0

            lax.fori_loop(lo, hi, unit, 0)

        def step(s, _):
            @pl.when(s < chunks)
            def _():
                wait_bytes(xb.at[s, :, end], xe_recv.at[s])

            @pl.when(s < chunks - 1)
            def _():
                remote(xb.at[s, :, end], xb.at[s, :, end], sent, xp_recv.at[s], (peer, j, i)).start()

            @pl.when(s == last)
            def _():
                tail_start(0)

            @pl.when((s == last) & (i % 2 == 0))
            def _():
                tail_start(1)

            @pl.when(s == 0)
            def _():
                forward(AHEAD, 0)

            @pl.when((s >= AHEAD) & (s + 1 < last))
            def _():
                forward(s + 1, 0)

            @pl.when(s == 0)
            def _():
                wait_bytes(a_ref, a_end)
                a_fan(a_unit(0, i, j), 0, i)
                a_start(a_unit(0, i, j), 0, i, j, a_x.at[0], (z, j, x_i))
                wait_bytes(a_ref, a_x.at[1])
                a_fan(a_unit(1, x_i, j), 1, x_i)

            def a_turn(e, k):
                wait_bytes(a_ref, a_y.at[e, k])
                row = x_i if k else i
                a_start(a_unit(e, row, 1 - j), e, row, 1 - j, a_core, (z, j, core_i))

            @pl.when(s == 1)
            def _():
                a_turn(1, 0)

            @pl.when(s == 2)
            def _():
                wait_bytes(a_ref, a_x.at[0])
                a_fan(a_unit(0, x_i, j), 0, x_i)
                a_turn(0, 0)

            @pl.when(s == LAG - 1)
            def _():
                a_turn(1, 1)
                a_turn(0, 1)
                wait_bytes(a_unit(1, i, j), kept)
                pl.semaphore_wait(ready, 4)
                wait_bytes(xb.at[:, 0, 0], kept)
                wait_bytes(ab.at[0], a_core)

            @pl.when(s >= LAG)
            def _():
                wait_bytes(xb.at[s - LAG, :, pl.ds(0, 2)], xp_recv.at[s - LAG])
                compute(s - LAG, 0, width)

            return 0

        lax.fori_loop(0, chunks + LAG - 1, step, 0)
        wait_bytes(xb.at[pl.ds(0, 8), 0, 0, :, pl.ds(0, narrow)], xt_recv.at[0])
        compute(last, 0, narrow, 0, 5)

        @pl.when(i % 2 == 1)
        def _():
            tail_start(1)

        compute(last, 0, narrow, 5, 8)
        wait_bytes(xb.at[pl.ds(0, 6), 0, 0, :, pl.ds(0, narrow)], xt_recv.at[1])
        rhs_part = xb[last, :2, :, :, pl.ds(narrow, narrow)].reshape(8 * rows, narrow)
        lhs_part = ab[0, :, :, : 8 * rows].reshape(4 * rows, 8 * rows)
        acc[...] = jnp.dot(lhs_part, rhs_part, preferred_element_type=jnp.float32).reshape(4, rows, narrow)
        wait_bytes(tail_part(2), xt_recv.at[2])
        compute(last, narrow, narrow, 0, 4, 2)
        compute(last, narrow, narrow, 4, 8)
        wait_bytes(x_ref.at[:, :, pl.ds(0, 3 * quarter)], sent)
        wait_bytes(ab.at[:, pl.ds(0, 3)], sent)
        wait_bytes(ab.at[0, 0], sent)
        wait_bytes(xb.at[:, :, pl.ds(0, 2)], sent)
        wait_bytes(yb.at[:, 0], sent)
        wait_bytes(yb.at[:, 1, pl.ds(0, 3)], sent)
        wait_bytes(yb.at[:, 1, 0], yl_sem)
        wait_bytes(o_ref.at[:, :, pl.ds(0, 3 * quarter)], y_recv)


def solution(mesh):
    def local_product(a, x):
        rhs, rows, cols = x.shape
        width = WIDTH
        while (cols // 4) % width:
            width //= 2
        chunks = rhs * (cols // 4 // width)
        dma = pltpu.SemaphoreType.DMA
        return pl.pallas_call(
            functools.partial(kernel, width),
            out_shape=pltpu.VMEM(x.shape, x.dtype),
            in_specs=[pl.BlockSpec(memory_space=pltpu.HBM)] * 2,
            out_specs=pl.BlockSpec(memory_space=pltpu.VMEM),
            scratch_shapes=[
                pltpu.VMEM((chunks, 4, 4, rows, width), x.dtype),
                pltpu.VMEM((2, 4, rows, 2 * a.shape[1]), a.dtype),
                pltpu.VMEM((chunks, 2, 4, rows, width), x.dtype),
                pltpu.VMEM((4, rows, width // 2), jnp.float32),
                dma, dma((4,)), dma((AHEAD - 1 + (chunks - AHEAD + 1) // 2,)), dma,
                dma((chunks,)), dma((chunks - 1,)), dma((3,)),
                dma, dma((2,)), dma((2, 2)), dma,
                dma, dma, pltpu.SemaphoreType.REGULAR, pltpu.SemaphoreType.REGULAR, pltpu.SemaphoreType.REGULAR, pltpu.SemaphoreType.REGULAR,
            ],
            compiler_params=pltpu.CompilerParams(collective_id=0, has_side_effects=True, vmem_limit_bytes=int(56.5 * 2**20)),
        )(x, a)

    return jax.shard_map(local_product, mesh=mesh, in_specs=(P(("row", "depth"), "col"), P(None, ("row", "depth"), "col")), out_specs=P(None, ("row", "depth"), "col"), check_vma=False)
```

```python
import functools

import jax
import jax.numpy as jnp
from jax import lax
from jax.experimental import pallas as pl
from jax.experimental.pallas import tpu as pltpu
from jax.sharding import PartitionSpec as P

MESH = pl.DeviceIdType.MESH
WIDTH = 256
AHEAD = 3
LAG = 4
BLOCKS = ((0, 3), (3, 1))


def kernel(width, x_ref, a_ref, o_ref, xb, ab, yb, acc, sent, xa_first, xa_recv, kept, xe_recv, xp_recv, xt_recv, a_end, a_x, a_y, a_core, y_recv, yl_sem, ready_core, ready_x, ready_y, ready):
    z = lax.axis_index("depth")
    j = lax.axis_index("col")
    i = lax.axis_index("row")
    rhs, rows, cols = x_ref.shape
    quarter = cols // 4
    subs = quarter // width
    chunks = rhs * subs
    last, narrow = chunks - 1, width // 2
    half = a_ref.shape[1]
    is_mid = (z + 1) // 2 == 1
    end = (z // 2) * 3
    near = 1 + z // 2
    peer = 3 - z
    core_i = i + 1 - 2 * (i % 2)
    x_i = (i + 2) % 4
    other_i = (core_i + 2) % 4

    def span(owner, sub):
        return pl.ds(pl.multiple_of(owner * quarter + sub * width, width), width)

    def a_unit(e, row, col):
        return ab.at[e, row, :, pl.ds(pl.multiple_of(col * half, half), half)]

    def remote(src, dst, send, recv, where):
        return pltpu.make_async_remote_copy(src_ref=src, dst_ref=dst, send_sem=send, recv_sem=recv, device_id=where, device_id_type=MESH)

    def wait_bytes(ref, sem):
        pltpu.make_async_copy(ref, ref, sem).wait()

    def early(c):
        return isinstance(c, int) and c < AHEAD

    def swap_slot(c):
        return xa_recv.at[c - 1 if early(c) else AHEAD - 1 + (c - AHEAD) // 2]

    def swap_start(c):
        r, sub = c // subs, c % subs
        arrived = xa_first.at[i] if early(c) and c == 0 else swap_slot(c)
        for to in (core_i, x_i, other_i):
            remote(x_ref.at[r, :, span(to, sub)], xb.at[c, i, z], sent, arrived, (z, j, to)).start()

    def own_start(c, to, arrived):
        r, sub = c // subs, c % subs
        remote(x_ref.at[r, :, span(i, sub)], xb.at[c, i, z], sent, arrived.at[c], (to, j, i)).start()

    def pass_on(c, to, arrived):
        if early(c):
            if c:
                wait_bytes(xb.at[c, pl.ds(0, 3), z], swap_slot(c))
        else:
            opens = (c - AHEAD) % 2 == 0

            @pl.when(jnp.logical_and(opens, c < last))
            def _():
                wait_bytes(xb.at[pl.ds(0, 2), pl.ds(0, 3), z], swap_slot(c))

            @pl.when(jnp.logical_and(opens, c == last))
            def _():
                wait_bytes(xb.at[c, pl.ds(0, 3), z], swap_slot(c))

        for t in (core_i, x_i, other_i):
            if early(c) and c == 0:
                wait_bytes(xb.at[c, t, z], xa_first.at[t])
            remote(xb.at[c, t, z], xb.at[c, t, z], sent, arrived.at[c], (to, j, i)).start()

    def tail_start(h):
        if h == 0:
            wait_bytes(xb.at[last, pl.ds(0, 3), z], swap_slot(last))
        for n, (at, size) in enumerate(BLOCKS if h else ((0, 4),)):
            for layer in (z, end):
                part = xb.at[last, pl.ds(at, size), layer, :, pl.ds(h * narrow, narrow)]
                remote(part, part, sent, xt_recv.at[n + h], (peer, j, i)).start()

    def a_start(src, e, row, col, arrived, where):
        remote(src, a_unit(e, row, col), sent, arrived, where).start()

    def notify(sem, where):
        pl.semaphore_signal(sem, inc=1, device_id=where, device_id_type=MESH)

    barrier = pltpu.get_barrier_semaphore()

    @pl.when(is_mid)
    def _():
        notify(barrier, (peer, j, i))

        @pl.when(i % 2 == 0)
        def _():
            notify(barrier, (z, j, core_i))

        @pl.when(i < 2)
        def _():
            for to in (x_i, other_i):
                notify(barrier, (z, j, to))

        @pl.when(j == 0)
        def _():
            notify(barrier, (z, 1, i))

        pl.semaphore_wait(barrier, 1 + i % 2 + i // 2 * 2 + j)

    @pl.when(jnp.logical_not(is_mid))
    def _():
        for d in (1, 2, 3):
            notify(barrier, (z, j, (i + d) % 4))
        pl.semaphore_wait(barrier, 7)

    @pl.when(jnp.logical_not(is_mid))
    def _():
        swap_start(0)
        a_start(a_ref, 0, i, j, a_end, (near, j, i))
        own_start(0, near, xe_recv)
        for t in range(4):
            notify(ready, (near, j, t))

        def issue(c, _):
            swap_start(c)
            own_start(c, near, xe_recv)
            return 0

        for c in range(1, AHEAD):
            issue(c, 0)

        def step(c, _):
            @pl.when(c + AHEAD < chunks)
            def _():
                issue(c + AHEAD, 0)

            pass_on(c, near, xe_recv)
            return 0

        for c in range(AHEAD):
            step(c, 0)
        lax.fori_loop(AHEAD, chunks, step, 0)
        wait_bytes(x_ref.at[:, :, pl.ds(0, 3 * quarter)], sent)
        wait_bytes(a_ref, sent)
        wait_bytes(xb.at[:, :, 0], sent)
        wait_bytes(o_ref, y_recv)

    @pl.when(is_mid)
    def _():
        def a_fan(src, e, row):
            a_start(src, e, row, j, a_y.at[e, 0 if row is i else 1], (z, 1 - j, i))
            a_start(src, e, row, j, a_core, (z, j, core_i))

        def issue(c, _):
            swap_start(c)

            @pl.when(c < last)
            def _():
                own_start(c, peer, xp_recv)

            return 0

        def first(c, _):
            own_start(c, peer, xp_recv)
            return 0

        lax.fori_loop(0, AHEAD, first, 0)
        for t in range(4):
            notify(barrier, (end, j, t))

        @pl.when(i % 2 == 1)
        def _():
            notify(ready_core, (z, j, core_i))

        @pl.when(i >= 2)
        def _():
            for to in (x_i, other_i):
                notify(ready_x, (z, j, to))

        @pl.when(j == 1)
        def _():
            notify(ready_y, (z, 0, i))

        @pl.when(i % 2 == 0)
        def _():
            pl.semaphore_wait(ready_core, 1)

        @pl.when(i < 2)
        def _():
            pl.semaphore_wait(ready_x, 2)

        swap_start(0)

        @pl.when(j == 0)
        def _():
            pl.semaphore_wait(ready_y, 1)

        a_fan(a_ref, 1, i)
        for c in range(1, AHEAD):
            swap_start(c)
        a_start(a_ref, 1, i, j, a_x.at[1], (z, j, x_i))
        pltpu.make_async_copy(a_ref, a_unit(1, i, j), kept).start()

        def keep(c, _):
            pltpu.make_async_copy(x_ref.at[c // subs, :, span(i, c % subs)], xb.at[c, i, z], kept).start()
            return 0

        lax.fori_loop(0, chunks, keep, 0)

        def forward(c, _):
            @pl.when(c + AHEAD < chunks)
            def _():
                issue(c + AHEAD, 0)

            pass_on(c, peer, xp_recv)
            return 0

        for c in range(AHEAD):
            forward(c, 0)

        def compute(c, at, size, lo=0, hi=8, done=0):
            r, sub = c // subs, c % subs
            cut = pl.ds(at, size)
            out = pl.ds(pl.multiple_of(i * quarter + sub * width + at, size), size)

            def unit(u, _):
                e, t = u // 4, u % 4
                block = xb[c, done:, :, :, cut].reshape((4 - done) * 4 * rows, size)
                total = jnp.dot(ab[e, t, :, done * 4 * rows :], block, preferred_element_type=jnp.float32)
                if done:
                    total = total + acc[t]
                yb[c, e, t, :, cut] = total.astype(yb.dtype)
                layer = end + e * (z - end)
                mine = (e == 1) & (t == i)

                @pl.when(mine)
                def _():
                    pltpu.make_async_copy(yb.at[c, e, t, :, cut], o_ref.at[r, :, out], yl_sem).start()

                @pl.when(jnp.logical_not(mine))
                def _():
                    remote(yb.at[c, e, t, :, cut], o_ref.at[r, :, out], sent, y_recv, (layer, j, t)).start()

                return 0

            lax.fori_loop(lo, hi, unit, 0)

        def step(s, _):
            @pl.when(s < chunks)
            def _():
                wait_bytes(xb.at[s, :, end], xe_recv.at[s])

            @pl.when(s < chunks - 1)
            def _():
                remote(xb.at[s, :, end], xb.at[s, :, end], sent, xp_recv.at[s], (peer, j, i)).start()

            @pl.when(s == last)
            def _():
                tail_start(0)

            @pl.when((s == last) & (i % 2 == 0))
            def _():
                tail_start(1)

            @pl.when(s == 0)
            def _():
                forward(AHEAD, 0)

            @pl.when((s >= AHEAD) & (s + 1 < last))
            def _():
                forward(s + 1, 0)

            @pl.when(s == 0)
            def _():
                wait_bytes(a_ref, a_end)
                a_fan(a_unit(0, i, j), 0, i)
                a_start(a_unit(0, i, j), 0, i, j, a_x.at[0], (z, j, x_i))
                wait_bytes(a_ref, a_x.at[1])
                a_fan(a_unit(1, x_i, j), 1, x_i)

            def a_turn(e, k):
                wait_bytes(a_ref, a_y.at[e, k])
                row = x_i if k else i
                a_start(a_unit(e, row, 1 - j), e, row, 1 - j, a_core, (z, j, core_i))

            @pl.when(s == 1)
            def _():
                a_turn(1, 0)

            @pl.when(s == 2)
            def _():
                wait_bytes(a_ref, a_x.at[0])
                a_fan(a_unit(0, x_i, j), 0, x_i)
                a_turn(0, 0)

            @pl.when(s == LAG - 1)
            def _():
                a_turn(1, 1)
                a_turn(0, 1)
                wait_bytes(a_unit(1, i, j), kept)
                pl.semaphore_wait(ready, 4)
                wait_bytes(xb.at[:, 0, 0], kept)
                wait_bytes(ab.at[0], a_core)

            @pl.when(s >= LAG)
            def _():
                wait_bytes(xb.at[s - LAG, :, pl.ds(0, 2)], xp_recv.at[s - LAG])
                compute(s - LAG, 0, width)

            return 0

        lax.fori_loop(0, chunks + LAG - 1, step, 0)
        wait_bytes(xb.at[pl.ds(0, 8), 0, 0, :, pl.ds(0, narrow)], xt_recv.at[0])
        compute(last, 0, narrow, 0, 5)

        @pl.when(i % 2 == 1)
        def _():
            tail_start(1)

        compute(last, 0, narrow, 5, 8)
        for n, (at, size) in enumerate(BLOCKS):
            wait_bytes(xb.at[pl.ds(0, 2 * size), 0, 0, :, pl.ds(0, narrow)], xt_recv.at[n + 1])
            if at + size < 4:
                rhs_part = xb[last, at : at + size, :, :, pl.ds(narrow, narrow)].reshape(4 * size * rows, narrow)
                lhs_part = ab[0, :, :, 4 * at * rows : 4 * (at + size) * rows].reshape(4 * rows, 4 * size * rows)
                sums = jnp.dot(lhs_part, rhs_part, preferred_element_type=jnp.float32).reshape(4, rows, narrow)
                acc[...] = acc[...] + sums if at else sums
        compute(last, narrow, narrow, 0, 4, BLOCKS[-1][0])
        compute(last, narrow, narrow, 4, 8)
        wait_bytes(x_ref.at[:, :, pl.ds(0, 3 * quarter)], sent)
        wait_bytes(ab.at[:, pl.ds(0, 3)], sent)
        wait_bytes(ab.at[0, 0], sent)
        wait_bytes(xb.at[:, :, pl.ds(0, 2)], sent)
        wait_bytes(yb.at[:, 0], sent)
        wait_bytes(yb.at[:, 1, pl.ds(0, 3)], sent)
        wait_bytes(yb.at[:, 1, 0], yl_sem)
        wait_bytes(o_ref.at[:, :, pl.ds(0, 3 * quarter)], y_recv)


def solution(mesh):
    def local_product(a, x):
        rhs, rows, cols = x.shape
        width = WIDTH
        while (cols // 4) % width:
            width //= 2
        chunks = rhs * (cols // 4 // width)
        dma = pltpu.SemaphoreType.DMA
        return pl.pallas_call(
            functools.partial(kernel, width),
            out_shape=pltpu.VMEM(x.shape, x.dtype),
            in_specs=[pl.BlockSpec(memory_space=pltpu.HBM)] * 2,
            out_specs=pl.BlockSpec(memory_space=pltpu.VMEM),
            scratch_shapes=[
                pltpu.VMEM((chunks, 4, 4, rows, width), x.dtype),
                pltpu.VMEM((2, 4, rows, 2 * a.shape[1]), a.dtype),
                pltpu.VMEM((chunks, 2, 4, rows, width), x.dtype),
                pltpu.VMEM((4, rows, width // 2), jnp.float32),
                dma, dma((4,)), dma((AHEAD - 1 + (chunks - AHEAD + 1) // 2,)), dma,
                dma((chunks,)), dma((chunks - 1,)), dma((1 + len(BLOCKS),)),
                dma, dma((2,)), dma((2, 2)), dma,
                dma, dma, pltpu.SemaphoreType.REGULAR, pltpu.SemaphoreType.REGULAR, pltpu.SemaphoreType.REGULAR, pltpu.SemaphoreType.REGULAR,
            ],
            compiler_params=pltpu.CompilerParams(collective_id=0, has_side_effects=True, vmem_limit_bytes=int(56.5 * 2**20)),
        )(x, a)

    return jax.shard_map(local_product, mesh=mesh, in_specs=(P(("row", "depth"), "col"), P(None, ("row", "depth"), "col")), out_specs=P(None, ("row", "depth"), "col"), check_vma=False)
```

```python
import functools

import jax
import jax.numpy as jnp
from jax import lax
from jax.experimental import pallas as pl
from jax.experimental.pallas import tpu as pltpu
from jax.sharding import PartitionSpec as P

MESH = pl.DeviceIdType.MESH
WIDTH = 256
AHEAD = 3
LAG = 4
BLOCKS = ((0, 3), (3, 1))


def kernel(width, x_ref, a_ref, o_ref, xb, ab, yb, acc, sent, xa_first, xa_recv, kept, xe_recv, xp_recv, xt_recv, a_end, a_x, a_y, a_core, y_recv, ready_mid, ready):
    z = lax.axis_index("depth")
    j = lax.axis_index("col")
    i = lax.axis_index("row")
    rhs, rows, cols = x_ref.shape
    quarter = cols // 4
    subs = quarter // width
    chunks = rhs * subs
    last, narrow = chunks - 1, width // 2
    half = a_ref.shape[1]
    is_mid = (z + 1) // 2 == 1
    end = (z // 2) * 3
    near = 1 + z // 2
    peer = 3 - z
    core_i = i + 1 - 2 * (i % 2)
    x_i = (i + 2) % 4
    other_i = (core_i + 2) % 4

    def span(owner, sub):
        return pl.ds(pl.multiple_of(owner * quarter + sub * width, width), width)

    def a_unit(e, row, col):
        return ab.at[e, row, :, pl.ds(pl.multiple_of(col * half, half), half)]

    def remote(src, dst, send, recv, where):
        return pltpu.make_async_remote_copy(src_ref=src, dst_ref=dst, send_sem=send, recv_sem=recv, device_id=where, device_id_type=MESH)

    def wait_bytes(ref, sem):
        pltpu.make_async_copy(ref, ref, sem).wait()

    def early(c):
        return isinstance(c, int) and c < AHEAD

    def swap_slot(c):
        return xa_recv.at[c - 1 if early(c) else AHEAD - 1 + (c - AHEAD) // 2]

    def swap_start(c):
        r, sub = c // subs, c % subs
        arrived = xa_first.at[i] if early(c) and c == 0 else swap_slot(c)
        for to in (core_i, x_i, other_i):
            remote(x_ref.at[r, :, span(to, sub)], xb.at[c, i, z], sent, arrived, (z, j, to)).start()

    def own_start(c, to, arrived):
        r, sub = c // subs, c % subs
        remote(x_ref.at[r, :, span(i, sub)], xb.at[c, i, z], sent, arrived.at[c], (to, j, i)).start()

    def pass_on(c, to, arrived):
        if early(c):
            if c:
                wait_bytes(xb.at[c, pl.ds(0, 3), z], swap_slot(c))
        else:
            opens = (c - AHEAD) % 2 == 0

            @pl.when(jnp.logical_and(opens, c < last))
            def _():
                wait_bytes(xb.at[pl.ds(0, 2), pl.ds(0, 3), z], swap_slot(c))

            @pl.when(jnp.logical_and(opens, c == last))
            def _():
                wait_bytes(xb.at[c, pl.ds(0, 3), z], swap_slot(c))

        for t in (core_i, x_i, other_i):
            if early(c) and c == 0:
                wait_bytes(xb.at[c, t, z], xa_first.at[t])
            remote(xb.at[c, t, z], xb.at[c, t, z], sent, arrived.at[c], (to, j, i)).start()

    def tail_start(h):
        if h == 0:
            wait_bytes(xb.at[last, pl.ds(0, 3), z], swap_slot(last))
        for n, (at, size) in enumerate(BLOCKS if h else ((0, 4),)):
            for layer in (z, end):
                part = xb.at[last, pl.ds(at, size), layer, :, pl.ds(h * narrow, narrow)]
                remote(part, part, sent, xt_recv.at[n + h], (peer, j, i)).start()

    def a_start(src, e, row, col, arrived, where):
        remote(src, a_unit(e, row, col), sent, arrived, where).start()

    def notify(sem, where):
        pl.semaphore_signal(sem, inc=1, device_id=where, device_id_type=MESH)

    barrier = pltpu.get_barrier_semaphore()

    @pl.when(is_mid)
    def _():
        notify(barrier, (peer, j, i))

        @pl.when(i % 2 == 0)
        def _():
            notify(barrier, (z, j, core_i))

        @pl.when(i < 2)
        def _():
            for to in (x_i, other_i):
                notify(barrier, (z, j, to))

        @pl.when(j == 0)
        def _():
            notify(barrier, (z, 1, i))

        pl.semaphore_wait(barrier, 1 + i % 2 + i // 2 * 2 + j)

    @pl.when(jnp.logical_not(is_mid))
    def _():
        for d in (1, 2, 3):
            notify(barrier, (z, j, (i + d) % 4))
        pl.semaphore_wait(barrier, 7)

    @pl.when(jnp.logical_not(is_mid))
    def _():
        swap_start(0)
        a_start(a_ref, 0, i, j, a_end, (near, j, i))
        own_start(0, near, xe_recv)
        for t in range(4):
            notify(ready, (near, j, t))

        def issue(c, _):
            swap_start(c)
            own_start(c, near, xe_recv)
            return 0

        for c in range(1, AHEAD):
            issue(c, 0)

        def step(c, _):
            @pl.when(c + AHEAD < chunks)
            def _():
                issue(c + AHEAD, 0)

            pass_on(c, near, xe_recv)
            return 0

        for c in range(AHEAD):
            step(c, 0)
        lax.fori_loop(AHEAD, chunks, step, 0)
        wait_bytes(x_ref.at[:, :, pl.ds(0, 3 * quarter)], sent)
        wait_bytes(a_ref, sent)
        wait_bytes(xb.at[:, :, 0], sent)
        wait_bytes(o_ref, y_recv)

    @pl.when(is_mid)
    def _():
        def a_fan(src, e, row):
            a_start(src, e, row, j, a_y.at[e, 0 if row is i else 1], (z, 1 - j, i))
            a_start(src, e, row, j, a_core, (z, j, core_i))

        def issue(c, _):
            swap_start(c)

            @pl.when(c < last)
            def _():
                own_start(c, peer, xp_recv)

            return 0

        def first(c, _):
            own_start(c, peer, xp_recv)
            return 0

        lax.fori_loop(0, AHEAD, first, 0)
        for t in range(4):
            notify(barrier, (end, j, t))

        @pl.when(i % 2 == 1)
        def _():
            notify(ready_mid, (z, j, core_i))

        @pl.when(i >= 2)
        def _():
            for to in (x_i, other_i):
                notify(ready_mid, (z, j, to))

        @pl.when(j == 1)
        def _():
            notify(ready_mid, (z, 0, i))

        @pl.when(i + j < 4)
        def _():
            pl.semaphore_wait(ready_mid, 1 - i % 2 + 2 - i // 2 * 2 + 1 - j)

        swap_start(0)
        a_fan(a_ref, 1, i)
        for c in range(1, AHEAD):
            swap_start(c)
        a_start(a_ref, 1, i, j, a_x.at[1], (z, j, x_i))
        pltpu.make_async_copy(a_ref, a_unit(1, i, j), kept).start()

        def keep(c, _):
            pltpu.make_async_copy(x_ref.at[c // subs, :, span(i, c % subs)], xb.at[c, i, z], kept).start()
            return 0

        lax.fori_loop(0, chunks, keep, 0)

        def forward(c, _):
            @pl.when(c + AHEAD < chunks)
            def _():
                issue(c + AHEAD, 0)

            pass_on(c, peer, xp_recv)
            return 0

        for c in range(AHEAD):
            forward(c, 0)

        def compute(c, at, size, lo=0, hi=8, done=0):
            r, sub = c // subs, c % subs
            cut = pl.ds(at, size)
            out = pl.ds(pl.multiple_of(i * quarter + sub * width + at, size), size)

            def unit(u, _):
                e, t = u // 4, u % 4
                block = xb[c, done:, :, :, cut].reshape((4 - done) * 4 * rows, size)
                total = jnp.dot(ab[e, t, :, done * 4 * rows :], block, preferred_element_type=jnp.float32)
                if done:
                    total = total + acc[t]
                yb[c, e, t, :, cut] = total.astype(yb.dtype)
                layer = end + e * (z - end)
                mine = (e == 1) & (t == i)

                @pl.when(mine)
                def _():
                    pltpu.make_async_copy(yb.at[c, e, t, :, cut], o_ref.at[r, :, out], kept).start()

                @pl.when(jnp.logical_not(mine))
                def _():
                    remote(yb.at[c, e, t, :, cut], o_ref.at[r, :, out], sent, y_recv, (layer, j, t)).start()

                return 0

            lax.fori_loop(lo, hi, unit, 0)

        def step(s, _):
            @pl.when(s < chunks)
            def _():
                wait_bytes(xb.at[s, :, end], xe_recv.at[s])

            @pl.when(s < chunks - 1)
            def _():
                remote(xb.at[s, :, end], xb.at[s, :, end], sent, xp_recv.at[s], (peer, j, i)).start()

            @pl.when(s == last)
            def _():
                tail_start(0)

            @pl.when((s == last) & (i % 2 == 0))
            def _():
                tail_start(1)

            @pl.when(s == 0)
            def _():
                forward(AHEAD, 0)

            @pl.when((s >= AHEAD) & (s + 1 < last))
            def _():
                forward(s + 1, 0)

            @pl.when(s == 0)
            def _():
                wait_bytes(a_ref, a_end)
                a_fan(a_unit(0, i, j), 0, i)
                a_start(a_unit(0, i, j), 0, i, j, a_x.at[0], (z, j, x_i))
                wait_bytes(a_ref, a_x.at[1])
                a_fan(a_unit(1, x_i, j), 1, x_i)

            def a_turn(e, k):
                wait_bytes(a_ref, a_y.at[e, k])
                row = x_i if k else i
                a_start(a_unit(e, row, 1 - j), e, row, 1 - j, a_core, (z, j, core_i))

            @pl.when(s == 1)
            def _():
                a_turn(1, 0)

            @pl.when(s == 2)
            def _():
                wait_bytes(a_ref, a_x.at[0])
                a_fan(a_unit(0, x_i, j), 0, x_i)
                a_turn(0, 0)

            @pl.when(s == LAG - 1)
            def _():
                a_turn(1, 1)
                a_turn(0, 1)
                wait_bytes(a_unit(1, i, j), kept)
                pl.semaphore_wait(ready, 4)
                wait_bytes(xb.at[:, 0, 0], kept)
                wait_bytes(ab.at[0], a_core)

            @pl.when(s >= LAG)
            def _():
                wait_bytes(xb.at[s - LAG, :, pl.ds(0, 2)], xp_recv.at[s - LAG])
                compute(s - LAG, 0, width)

            return 0

        lax.fori_loop(0, chunks + LAG - 1, step, 0)
        wait_bytes(xb.at[pl.ds(0, 8), 0, 0, :, pl.ds(0, narrow)], xt_recv.at[0])
        compute(last, 0, narrow, 0, 5)

        @pl.when(i % 2 == 1)
        def _():
            tail_start(1)

        compute(last, 0, narrow, 5, 8)
        for n, (at, size) in enumerate(BLOCKS):
            wait_bytes(xb.at[pl.ds(0, 2 * size), 0, 0, :, pl.ds(0, narrow)], xt_recv.at[n + 1])
            if at + size < 4:
                rhs_part = xb[last, at : at + size, :, :, pl.ds(narrow, narrow)].reshape(4 * size * rows, narrow)
                lhs_part = ab[0, :, :, 4 * at * rows : 4 * (at + size) * rows].reshape(4 * rows, 4 * size * rows)
                sums = jnp.dot(lhs_part, rhs_part, preferred_element_type=jnp.float32).reshape(4, rows, narrow)
                acc[...] = acc[...] + sums if at else sums
        compute(last, narrow, narrow, 0, 4, BLOCKS[-1][0])
        compute(last, narrow, narrow, 4, 8)
        wait_bytes(x_ref.at[:, :, pl.ds(0, 3 * quarter)], sent)
        wait_bytes(ab.at[:, pl.ds(0, 3)], sent)
        wait_bytes(ab.at[0, 0], sent)
        wait_bytes(xb.at[:, :, pl.ds(0, 2)], sent)
        wait_bytes(yb.at[:, 0], sent)
        wait_bytes(yb.at[:, 1, pl.ds(0, 3)], sent)
        wait_bytes(yb.at[:, 1, 0], kept)
        wait_bytes(o_ref.at[:, :, pl.ds(0, 3 * quarter)], y_recv)


def solution(mesh):
    def local_product(a, x):
        rhs, rows, cols = x.shape
        width = WIDTH
        while (cols // 4) % width:
            width //= 2
        chunks = rhs * (cols // 4 // width)
        dma = pltpu.SemaphoreType.DMA
        return pl.pallas_call(
            functools.partial(kernel, width),
            out_shape=pltpu.VMEM(x.shape, x.dtype),
            in_specs=[pl.BlockSpec(memory_space=pltpu.HBM)] * 2,
            out_specs=pl.BlockSpec(memory_space=pltpu.VMEM),
            scratch_shapes=[
                pltpu.VMEM((chunks, 4, 4, rows, width), x.dtype),
                pltpu.VMEM((2, 4, rows, 2 * a.shape[1]), a.dtype),
                pltpu.VMEM((chunks, 2, 4, rows, width), x.dtype),
                pltpu.VMEM((4, rows, width // 2), jnp.float32),
                dma, dma((4,)), dma((AHEAD - 1 + (chunks - AHEAD + 1) // 2,)), dma,
                dma((chunks,)), dma((chunks - 1,)), dma((1 + len(BLOCKS),)),
                dma, dma((2,)), dma((2, 2)), dma,
                dma, pltpu.SemaphoreType.REGULAR, pltpu.SemaphoreType.REGULAR,
            ],
            compiler_params=pltpu.CompilerParams(collective_id=0, has_side_effects=True, vmem_limit_bytes=int(56.5 * 2**20)),
        )(x, a)

    return jax.shard_map(local_product, mesh=mesh, in_specs=(P(("row", "depth"), "col"), P(None, ("row", "depth"), "col")), out_specs=P(None, ("row", "depth"), "col"), check_vma=False)
```

```python
import functools

import jax
import jax.numpy as jnp
from jax import lax
from jax.experimental import pallas as pl
from jax.experimental.pallas import tpu as pltpu
from jax.sharding import PartitionSpec as P

MESH = pl.DeviceIdType.MESH
WIDTH = 256
AHEAD = 3
LAG = 4
BLOCKS = ((0, 3), (3, 1))


def kernel(width, x_ref, a_ref, o_ref, xb, ab, yb, acc, sent, xa_first, xa_recv, kept, xe_recv, xp_recv, xt_recv, a_end, a_x, a_y, a_core, y_recv, ready_mid, ready):
    z = lax.axis_index("depth")
    j = lax.axis_index("col")
    i = lax.axis_index("row")
    rhs, rows, cols = x_ref.shape
    quarter = cols // 4
    subs = quarter // width
    chunks = rhs * subs
    last, narrow = chunks - 1, width // 2
    half = a_ref.shape[1]
    is_mid = (z + 1) // 2 == 1
    end = (z // 2) * 3
    near = 1 + z // 2
    peer = 3 - z
    core_i = i + 1 - 2 * (i % 2)
    x_i = (i + 2) % 4
    other_i = (core_i + 2) % 4

    def span(owner, sub):
        return pl.ds(pl.multiple_of(owner * quarter + sub * width, width), width)

    def a_unit(e, row, col):
        return ab.at[e, row, :, pl.ds(pl.multiple_of(col * half, half), half)]

    def remote(src, dst, send, recv, where):
        return pltpu.make_async_remote_copy(src_ref=src, dst_ref=dst, send_sem=send, recv_sem=recv, device_id=where, device_id_type=MESH)

    def wait_bytes(ref, sem):
        pltpu.make_async_copy(ref, ref, sem).wait()

    def early(c):
        return isinstance(c, int) and c < AHEAD

    def swap_slot(c):
        return xa_recv.at[c - 1 if early(c) else AHEAD - 1 + (c - AHEAD) // 2]

    def swap_start(c):
        r, sub = c // subs, c % subs
        for to in (core_i, x_i, other_i):
            arrived = xa_first.at[(i - to + 4) % 4 - 1] if early(c) and c == 0 else swap_slot(c)
            remote(x_ref.at[r, :, span(to, sub)], xb.at[c, i, z], sent, arrived, (z, j, to)).start()

    def own_start(c, to, arrived):
        r, sub = c // subs, c % subs
        remote(x_ref.at[r, :, span(i, sub)], xb.at[c, i, z], sent, arrived.at[c], (to, j, i)).start()

    def pass_on(c, to, arrived):
        if early(c):
            if c:
                wait_bytes(xb.at[c, pl.ds(0, 3), z], swap_slot(c))
        else:
            opens = (c - AHEAD) % 2 == 0

            @pl.when(jnp.logical_and(opens, c < last))
            def _():
                wait_bytes(xb.at[pl.ds(0, 2), pl.ds(0, 3), z], swap_slot(c))

            @pl.when(jnp.logical_and(opens, c == last))
            def _():
                wait_bytes(xb.at[c, pl.ds(0, 3), z], swap_slot(c))

        for t in (core_i, x_i, other_i):
            if early(c) and c == 0:
                wait_bytes(xb.at[c, t, z], xa_first.at[(t - i + 4) % 4 - 1])
            remote(xb.at[c, t, z], xb.at[c, t, z], sent, arrived.at[c], (to, j, i)).start()

    def tail_start(h):
        if h == 0:
            wait_bytes(xb.at[last, pl.ds(0, 3), z], swap_slot(last))
        for n, (at, size) in enumerate(BLOCKS if h else ((0, 4),)):
            for layer in (z, end):
                part = xb.at[last, pl.ds(at, size), layer, :, pl.ds(h * narrow, narrow)]
                remote(part, part, sent, xt_recv.at[n + h], (peer, j, i)).start()

    def a_start(src, e, row, col, arrived, where):
        remote(src, a_unit(e, row, col), sent, arrived, where).start()

    def notify(sem, where):
        pl.semaphore_signal(sem, inc=1, device_id=where, device_id_type=MESH)

    barrier = pltpu.get_barrier_semaphore()

    @pl.when(is_mid)
    def _():
        notify(barrier, (peer, j, i))

        @pl.when(i % 2 == 0)
        def _():
            notify(barrier, (z, j, core_i))

        @pl.when(i < 2)
        def _():
            for to in (x_i, other_i):
                notify(barrier, (z, j, to))

        @pl.when(j == 0)
        def _():
            notify(barrier, (z, 1, i))

        pl.semaphore_wait(barrier, 1 + i % 2 + i // 2 * 2 + j)

    @pl.when(jnp.logical_not(is_mid))
    def _():
        for d in (1, 2, 3):
            notify(barrier, (z, j, (i + d) % 4))
        pl.semaphore_wait(barrier, 7)

    @pl.when(jnp.logical_not(is_mid))
    def _():
        swap_start(0)
        a_start(a_ref, 0, i, j, a_end, (near, j, i))
        own_start(0, near, xe_recv)
        for t in range(4):
            notify(ready, (near, j, t))

        def issue(c, _):
            swap_start(c)
            own_start(c, near, xe_recv)
            return 0

        for c in range(1, AHEAD):
            issue(c, 0)

        def step(c, _):
            @pl.when(c + AHEAD < chunks)
            def _():
                issue(c + AHEAD, 0)

            pass_on(c, near, xe_recv)
            return 0

        for c in range(AHEAD):
            step(c, 0)
        lax.fori_loop(AHEAD, chunks, step, 0)
        wait_bytes(x_ref.at[:, :, pl.ds(0, 3 * quarter)], sent)
        wait_bytes(a_ref, sent)
        wait_bytes(xb.at[:, :, 0], sent)
        wait_bytes(o_ref, y_recv)

    @pl.when(is_mid)
    def _():
        def a_fan(src, e, row):
            a_start(src, e, row, j, a_y.at[e, 0 if row is i else 1], (z, 1 - j, i))
            a_start(src, e, row, j, a_core, (z, j, core_i))

        def issue(c, _):
            swap_start(c)

            @pl.when(c < last)
            def _():
                own_start(c, peer, xp_recv)

            return 0

        def first(c, _):
            own_start(c, peer, xp_recv)
            return 0

        lax.fori_loop(0, AHEAD, first, 0)
        for t in range(4):
            notify(barrier, (end, j, t))

        @pl.when(i % 2 == 1)
        def _():
            notify(ready_mid, (z, j, core_i))

        @pl.when(i >= 2)
        def _():
            for to in (x_i, other_i):
                notify(ready_mid, (z, j, to))

        @pl.when(j == 1)
        def _():
            notify(ready_mid, (z, 0, i))

        @pl.when(i + j < 4)
        def _():
            pl.semaphore_wait(ready_mid, 1 - i % 2 + 2 - i // 2 * 2 + 1 - j)

        swap_start(0)
        a_fan(a_ref, 1, i)
        for c in range(1, AHEAD):
            swap_start(c)
        a_start(a_ref, 1, i, j, a_x.at[1], (z, j, x_i))
        pltpu.make_async_copy(a_ref, a_unit(1, i, j), kept).start()

        def keep(c, _):
            pltpu.make_async_copy(x_ref.at[c // subs, :, span(i, c % subs)], xb.at[c, i, z], kept).start()
            return 0

        lax.fori_loop(0, chunks, keep, 0)

        def forward(c, _):
            @pl.when(c + AHEAD < chunks)
            def _():
                issue(c + AHEAD, 0)

            pass_on(c, peer, xp_recv)
            return 0

        for c in range(AHEAD):
            forward(c, 0)

        def compute(c, at, size, lo=0, hi=8, done=0):
            r, sub = c // subs, c % subs
            cut = pl.ds(at, size)
            out = pl.ds(pl.multiple_of(i * quarter + sub * width + at, size), size)

            def unit(u, _):
                e, t = u // 4, u % 4
                block = xb[c, done:, :, :, cut].reshape((4 - done) * 4 * rows, size)
                total = jnp.dot(ab[e, t, :, done * 4 * rows :], block, preferred_element_type=jnp.float32)
                if done:
                    total = total + acc[t]
                yb[c, e, t, :, cut] = total.astype(yb.dtype)
                layer = end + e * (z - end)
                mine = (e == 1) & (t == i)

                @pl.when(mine)
                def _():
                    pltpu.make_async_copy(yb.at[c, e, t, :, cut], o_ref.at[r, :, out], kept).start()

                @pl.when(jnp.logical_not(mine))
                def _():
                    remote(yb.at[c, e, t, :, cut], o_ref.at[r, :, out], sent, y_recv, (layer, j, t)).start()

                return 0

            lax.fori_loop(lo, hi, unit, 0)

        def step(s, _):
            @pl.when(s < chunks)
            def _():
                wait_bytes(xb.at[s, :, end], xe_recv.at[s])

            @pl.when(s < chunks - 1)
            def _():
                remote(xb.at[s, :, end], xb.at[s, :, end], sent, xp_recv.at[s], (peer, j, i)).start()

            @pl.when(s == last)
            def _():
                tail_start(0)

            @pl.when((s == last) & (i % 2 == 0))
            def _():
                tail_start(1)

            @pl.when(s == 0)
            def _():
                forward(AHEAD, 0)

            @pl.when((s >= AHEAD) & (s + 1 < last))
            def _():
                forward(s + 1, 0)

            @pl.when(s == 0)
            def _():
                wait_bytes(a_ref, a_end)
                a_fan(a_unit(0, i, j), 0, i)
                a_start(a_unit(0, i, j), 0, i, j, a_x.at[0], (z, j, x_i))
                wait_bytes(a_ref, a_x.at[1])
                a_fan(a_unit(1, x_i, j), 1, x_i)

            def a_turn(e, k):
                wait_bytes(a_ref, a_y.at[e, k])
                row = x_i if k else i
                a_start(a_unit(e, row, 1 - j), e, row, 1 - j, a_core, (z, j, core_i))

            @pl.when(s == 1)
            def _():
                a_turn(1, 0)

            @pl.when(s == 2)
            def _():
                wait_bytes(a_ref, a_x.at[0])
                a_fan(a_unit(0, x_i, j), 0, x_i)
                a_turn(0, 0)

            @pl.when(s == LAG - 1)
            def _():
                a_turn(1, 1)
                a_turn(0, 1)
                wait_bytes(a_unit(1, i, j), kept)
                pl.semaphore_wait(ready, 4)
                wait_bytes(xb.at[:, 0, 0], kept)
                wait_bytes(ab.at[0], a_core)

            @pl.when(s >= LAG)
            def _():
                wait_bytes(xb.at[s - LAG, :, pl.ds(0, 2)], xp_recv.at[s - LAG])
                compute(s - LAG, 0, width)

            return 0

        lax.fori_loop(0, chunks + LAG - 1, step, 0)
        wait_bytes(xb.at[pl.ds(0, 8), 0, 0, :, pl.ds(0, narrow)], xt_recv.at[0])
        compute(last, 0, narrow, 0, 5)

        @pl.when(i % 2 == 1)
        def _():
            tail_start(1)

        compute(last, 0, narrow, 5, 8)
        for n, (at, size) in enumerate(BLOCKS):
            wait_bytes(xb.at[pl.ds(0, 2 * size), 0, 0, :, pl.ds(0, narrow)], xt_recv.at[n + 1])
            if at + size < 4:
                rhs_part = xb[last, at : at + size, :, :, pl.ds(narrow, narrow)].reshape(4 * size * rows, narrow)
                lhs_part = ab[0, :, :, 4 * at * rows : 4 * (at + size) * rows].reshape(4 * rows, 4 * size * rows)
                sums = jnp.dot(lhs_part, rhs_part, preferred_element_type=jnp.float32).reshape(4, rows, narrow)
                acc[...] = acc[...] + sums if at else sums
        compute(last, narrow, narrow, 0, 4, BLOCKS[-1][0])
        compute(last, narrow, narrow, 4, 8)
        wait_bytes(x_ref.at[:, :, pl.ds(0, 3 * quarter)], sent)
        wait_bytes(ab.at[:, pl.ds(0, 3)], sent)
        wait_bytes(ab.at[0, 0], sent)
        wait_bytes(xb.at[:, :, pl.ds(0, 2)], sent)
        wait_bytes(yb.at[:, 0], sent)
        wait_bytes(yb.at[:, 1, pl.ds(0, 3)], sent)
        wait_bytes(yb.at[:, 1, 0], kept)
        wait_bytes(o_ref.at[:, :, pl.ds(0, 3 * quarter)], y_recv)


def solution(mesh):
    def local_product(a, x):
        rhs, rows, cols = x.shape
        width = WIDTH
        while (cols // 4) % width:
            width //= 2
        chunks = rhs * (cols // 4 // width)
        dma = pltpu.SemaphoreType.DMA
        return pl.pallas_call(
            functools.partial(kernel, width),
            out_shape=pltpu.VMEM(x.shape, x.dtype),
            in_specs=[pl.BlockSpec(memory_space=pltpu.HBM)] * 2,
            out_specs=pl.BlockSpec(memory_space=pltpu.VMEM),
            scratch_shapes=[
                pltpu.VMEM((chunks, 4, 4, rows, width), x.dtype),
                pltpu.VMEM((2, 4, rows, 2 * a.shape[1]), a.dtype),
                pltpu.VMEM((chunks, 2, 4, rows, width), x.dtype),
                pltpu.VMEM((4, rows, width // 2), jnp.float32),
                dma, dma((3,)), dma((AHEAD - 1 + (chunks - AHEAD + 1) // 2,)), dma,
                dma((chunks,)), dma((chunks - 1,)), dma((1 + len(BLOCKS),)),
                dma, dma((2,)), dma((2, 2)), dma,
                dma, pltpu.SemaphoreType.REGULAR, pltpu.SemaphoreType.REGULAR,
            ],
            compiler_params=pltpu.CompilerParams(collective_id=0, has_side_effects=True, vmem_limit_bytes=int(56.5 * 2**20)),
        )(x, a)

    return jax.shard_map(local_product, mesh=mesh, in_specs=(P(("row", "depth"), "col"), P(None, ("row", "depth"), "col")), out_specs=P(None, ("row", "depth"), "col"), check_vma=False)
```
